128 devices in a mesh: gx: 8 (over y, z_hi), gy: 8 (over x, core), gz: 2 (over z_lo).
Axes of the slice: x: 4, y: 4, z: 4 (z_hi: 2, z_lo: 2; z = z_hi * 2 + z_lo), core: 2. Of those that a mesh axis runs over, the one named last changes fastest.
Arguments:
- density: float32 [32, 256, 256], P('gx', 'gy', 'gz'), may hold values from 0.6 to 1.4
- velocity: float32 [3, 32, 256, 256], P(None, 'gx', 'gy', 'gz'), may hold values from -0.3 to 0.3
- solid_mask: int32 [32, 256, 256], P('gx', 'gy', 'gz'), may hold values 0 or 1
Outputs:
- density_final: float32 [32, 256, 256], P('gx', 'gy', 'gz')
- momentum: float32 [3, 32, 256, 256], P(None, 'gx', 'gy', 'gz')
The draws below stay inside these ranges and needn't reach their ends.
All inputs are finite; a program needn't handle non-finite values.
Results may differ from the reference program's by a relative error of at most 0.0003.
Values sent between devices are 32-bit elements.
A program may use at most 64 MiB of HBM per device.

```python
import jax
import jax.numpy as jnp
import numpy as np
from jax import lax

ITERS = 4
NX = 32
NY = 256
NZ = 256


def set_ends(result, key, low, largest):
    shape = result.shape
    place = [jax.random.randint(jax.random.fold_in(key, axis), (), 0, shape[axis]) for axis in range(len(shape))]
    result = result.at[tuple(place)].set(low)
    longest = shape.index(max(shape))
    place[longest] = (place[longest] + 1) % shape[longest]
    return result.at[tuple(place)].set(largest)


def block_levels(stream_key, dims, cuts, low, top_value):
    gain = 1.0
    for dim, shards_of in cuts:
        steps = jax.random.uniform(jax.random.fold_in(jax.random.fold_in(stream_key, 6), dim), (shards_of,), jnp.float32, low / len(cuts), top_value / len(cuts))
        gain = gain * jnp.repeat(jnp.exp(steps), dims[dim] // shards_of).reshape((-1,) + (1,) * (len(dims) - 1 - dim))
    return gain


def centred(key, dims, spread, most, shards=(), kind=jnp.bfloat16):
    result = spread * jax.random.normal(key, dims, jnp.float32)
    if shards:
        result = result * block_levels(key, dims, shards, -0.22, 0.18)
    return jnp.clip(result, -most, most).astype(kind)


def setup_inputs(seed: int = 0) -> dict:
    arg_keys = jax.random.split(jax.random.key(seed), 4)
    return {
        "density": jnp.clip(0.6 + 0.79999995 * jax.random.uniform(arg_keys[0], (NX, NY, NZ), jnp.float32) ** block_levels(arg_keys[0], (NX, NY, NZ), ((0, 8), (1, 8), (2, 2)), -0.2, 0.2), 0.6, 1.4),
        "velocity": centred(arg_keys[1], (3, NX, NY, NZ), 0.1, 0.3, ((1, 8), (2, 8), (3, 2)), jnp.float32),
        "solid_mask": set_ends((jax.random.randint(arg_keys[2], (NX, NY, NZ), 0, 10) < 1).astype(jnp.int32), jax.random.fold_in(arg_keys[2], 1), 0, 1),
    }


VELOCITIES = [(0, 0, 0), (1, 0, 0), (-1, 0, 0), (0, 1, 0), (0, -1, 0), (0, 0, 1), (0, 0, -1),
              (1, 1, 0), (-1, -1, 0), (1, -1, 0), (-1, 1, 0), (1, 0, 1), (-1, 0, -1),
              (1, 0, -1), (-1, 0, 1), (0, 1, 1), (0, -1, -1), (0, 1, -1), (0, -1, 1)]
WEIGHTS = [1.0 / 3.0] + [1.0 / 18.0] * 6 + [1.0 / 36.0] * 12
OPPOSITE = [0, 2, 1, 4, 3, 6, 5, 8, 7, 10, 9, 12, 11, 14, 13, 16, 15, 18, 17]
RELAX_RATE = 1.25


def equilibrium(density_now, velocity_now):
    velocity_table = jnp.asarray(np.array(VELOCITIES), jnp.float32)
    projected = jnp.tensordot(velocity_table, velocity_now, axes=1, precision=lax.Precision.HIGHEST)
    speed_sq = jnp.sum(velocity_now * velocity_now, axis=0)
    weights = jnp.asarray(np.array(WEIGHTS), jnp.float32).reshape((19, 1, 1, 1))
    return weights * density_now * (1.0 + 3.0 * projected + 4.5 * projected * projected - 1.5 * speed_sq)


def moments(fields):
    velocity_table = jnp.asarray(np.array(VELOCITIES), jnp.float32)
    density_now = jnp.sum(fields, axis=0)
    momentum_now = jnp.tensordot(velocity_table.T, fields, axes=1, precision=lax.Precision.HIGHEST)
    return density_now, momentum_now


def collide(fields, solid_mask):
    density_now, momentum_now = moments(fields)
    balance = equilibrium(density_now, momentum_now / density_now)
    relaxed = fields - RELAX_RATE * (fields - balance)
    bounced = fields[np.array(OPPOSITE)]
    return jnp.where(solid_mask[None] == 1, bounced, relaxed)


def reference(density, velocity, solid_mask):
    fields = equilibrium(density, velocity)
    for iteration in range(ITERS):
        collided = collide(fields, solid_mask)
        fields = jnp.stack([jnp.roll(collided[which_pop], VELOCITIES[which_pop], axis=(0, 1, 2))
                            for which_pop in range(19)])
    density_final, momentum = moments(fields)
    return density_final, momentum
```

```python
import jax
import jax.numpy as jnp
from jax import lax
from jax.experimental import pallas as pl
from jax.experimental.pallas import tpu as pltpu
from jax.sharding import PartitionSpec as P

MESH = pl.DeviceIdType.MESH

VELOCITIES = [
    (0, 0, 0),
    (1, 0, 0),
    (-1, 0, 0),
    (0, 1, 0),
    (0, -1, 0),
    (0, 0, 1),
    (0, 0, -1),
    (1, 1, 0),
    (-1, -1, 0),
    (1, -1, 0),
    (-1, 1, 0),
    (1, 0, 1),
    (-1, 0, -1),
    (1, 0, -1),
    (-1, 0, 1),
    (0, 1, 1),
    (0, -1, -1),
    (0, 1, -1),
    (0, -1, 1),
]
RELAX_RATE = 1.25
W0, W1, W2 = 1.0 / 3.0, 1.0 / 18.0, 1.0 / 36.0

G = 4
LAYERS, ROWS, LANES = 12, 48, 128
BLOCKS = [4 + 8 * j for j in range(5)]
INNER = [8 + 8 * j for j in range(4)]


def moments(f):
    s = [f[2 * k + 1] + f[2 * k + 2] for k in range(9)]
    d = [f[2 * k + 1] - f[2 * k + 2] for k in range(9)]
    rho = f[0] + (((s[0] + s[1]) + (s[2] + s[3])) + ((s[4] + s[5]) + (s[6] + s[7]))) + s[8]
    mx = d[0] + (d[3] + d[4]) + (d[5] + d[6])
    my = d[1] + (d[3] - d[4]) + (d[7] + d[8])
    mz = d[2] + (d[5] - d[6]) + (d[7] - d[8])
    return rho, mx, my, mz


def balance(rho, m, u, scale):
    mx, my, mz = m
    ux, uy, uz = u
    xx, yy, zz = mx * ux, my * uy, mz * uz
    base = rho - 1.5 * (xx + yy + zz)
    rest = (scale * W0) * base
    b1 = (scale * W1) * base
    b2 = (scale * W2) * base
    k1 = scale * W1 * 4.5
    k2 = scale * W2 * 4.5
    o1 = scale * W1 * 3.0
    o2 = scale * W2 * 3.0
    pairs = [(b1 + k1 * xx, o1 * mx), (b1 + k1 * yy, o1 * my), (b1 + k1 * zz, o1 * mz)]
    px, py, pz = o2 * mx, o2 * my, o2 * mz
    exx, eyy, ezz = k2 * xx, k2 * yy, k2 * zz
    cross_x, cross_y = (2.0 * k2) * mx, (2.0 * k2) * my
    for ea, eb, cross, pa, pb in (
        (exx, eyy, cross_x * uy, px, py),
        (exx, ezz, cross_x * uz, px, pz),
        (eyy, ezz, cross_y * uz, py, pz),
    ):
        even = b2 + (ea + eb)
        pairs.append((even + cross, pa + pb))
        pairs.append((even - cross, pa - pb))
    return rest, pairs


def first(rho, vx, vy, vz, solid):
    sign = jnp.where(solid, -1.0, 1.0)
    u = (vx * sign, vy * sign, vz * sign)
    m = tuple(rho * v for v in u)
    rest, pairs = balance(rho, m, u, 1.0)
    out = [rest]
    for even, odd in pairs:
        out += [even + odd, even - odd]
    return out


def collide(f, solid):
    rho, mx, my, mz = moments(f)
    inv = 1.0 / rho
    rest, pairs = balance(rho, (mx, my, mz), (mx * inv, my * inv, mz * inv), RELAX_RATE)
    keep = 1.0 - RELAX_RATE
    out = [jnp.where(solid, f[0], keep * f[0] + rest)]
    for k, (even, odd) in enumerate(pairs):
        a, b = f[2 * k + 1], f[2 * k + 2]
        out.append(jnp.where(solid, b, keep * a + (even + odd)))
        out.append(jnp.where(solid, a, keep * b + (even - odd)))
    return out


def kernel(
    density,
    velocity,
    mask,
    out_density,
    out_momentum,
    fld,
    msk,
    pack,
    peer,
    gfld,
    gmsk,
    main_a,
    main_b,
    side_a,
    side_b,
    load_sem,
    y_send,
    y_recv,
    z_send,
    z_recv,
    x_send,
    x_recv,
    f_send,
    f_recv,
):
    gx, gy, gz = lax.axis_index("gx"), lax.axis_index("gy"), lax.axis_index("gz")
    par = lax.rem(gx, 2)
    y_up = (gx, lax.rem(gy + 1, 8), gz)
    y_down = (gx, lax.rem(gy + 7, 8), gz)
    z_peer = (gx, gy, 1 - gz)
    x_peer = (gx + 1 - 2 * par, gy, gz)
    fwd_to = (lax.rem(gx + 2 + 4 * par, 8), gy, gz)
    fwd_from = (lax.rem(gx + 6 - 4 * par, 8), gy, gz)

    loads = [
        pltpu.make_async_copy(density, fld.at[0, 4:8, 8:40], load_sem.at[0]),
        pltpu.make_async_copy(velocity, fld.at[1:4, 4:8, 8:40], load_sem.at[1]),
        pltpu.make_async_copy(mask, msk.at[4:8, 8:40], load_sem.at[2]),
    ]
    for c in loads:
        c.start()

    barrier = pltpu.get_barrier_semaphore()
    for dev in (y_up, y_down, z_peer, x_peer, fwd_to, fwd_from):
        pl.semaphore_signal(barrier, inc=1, device_id=dev, device_id_type=MESH)
    pl.semaphore_wait(barrier, 6)
    for c in loads:
        c.wait()

    def remote(src, dst, send, recv, dev):
        return pltpu.make_async_remote_copy(
            src_ref=src, dst_ref=dst, send_sem=send, recv_sem=recv, device_id=dev, device_id_type=MESH
        )

    y_copies = [
        remote(fld.at[:, 4:8, 36:40], fld.at[:, 4:8, 4:8], y_send.at[0], y_recv.at[0], y_up),
        remote(fld.at[:, 4:8, 8:12], fld.at[:, 4:8, 40:44], y_send.at[1], y_recv.at[1], y_down),
        remote(msk.at[4:8, 36:40], msk.at[4:8, 4:8], y_send.at[2], y_recv.at[2], y_up),
        remote(msk.at[4:8, 8:12], msk.at[4:8, 40:44], y_send.at[3], y_recv.at[3], y_down),
    ]
    for c in y_copies:
        c.start()

    near = pl.ds(8 * (1 - par), 4)
    far = pl.ds(8 * par, 4)
    near_slot, far_slot = 2 * (1 - par), 2 * par

    def parts(layers, slot):
        refs = [fld.at[f, layers, 8:40] for f in range(4)] + [msk.at[layers, 8:40]]
        refs += [fld.at[:, layers, 4:8], fld.at[:, layers, 40:44], msk.at[layers, 4:8], msk.at[layers, 40:44]]
        refs += [peer.at[slot, :, 4:44]]
        return refs

    own = pl.ds(4, 4)
    x_copies = [
        remote(a, b, x_send.at[i], x_recv.at[i], x_peer)
        for i, (a, b) in enumerate(zip(parts(own, 1), parts(far, far_slot)))
    ]
    f_copies = [
        remote(a, b, f_send.at[i], f_recv.at[i], fwd_to)
        for i, (a, b) in enumerate(zip(parts(near, near_slot), parts(far, far_slot)))
    ]
    for c in x_copies[:5]:
        c.start()
    for c in y_copies:
        c.wait_recv()
    for c in x_copies[5:9]:
        c.start()

    lane = lax.broadcasted_iota(jnp.int32, (8, LANES), 1)
    group = lane // 8
    low_half = lax.rem(lane, 8) < 4

    for r in BLOCKS:
        rows = slice(r, r + 8)
        acc = None
        for f in range(4):
            for x in range(4):
                part = pltpu.roll(fld[f, 4 + x, rows], 32 * f + 8 * x + 4, 1)
                acc = part if acc is None else jnp.where(group == 4 * f + x, part, acc)
        pack[0, rows] = acc
        acc = None
        for x in range(4):
            part = pltpu.roll(msk[4 + x, rows].astype(jnp.float32), 8 * x + 4, 1)
            acc = part if acc is None else jnp.where(group == x, part, acc)
        pack[1, rows] = acc

    z_copy = remote(pack.at[:, 4:44], peer.at[1, :, 4:44], z_send, z_recv, z_peer)
    x_copies[0].wait_recv()
    f_copies[0].start()
    z_copy.start()
    z_copy.wait_recv()
    x_copies[9].start()
    for i in range(1, 10):
        x_copies[i].wait_recv()
        f_copies[i].start()
    for c in f_copies:
        c.wait_recv()

    def build_side(field, slot_part, slot_shift, store):
        for r in BLOCKS:
            rows = slice(r, r + 8)
            mine = None
            for x in range(LAYERS):
                part = pltpu.roll(field(x, rows), 8 * x + 4, 1)
                mine = part if mine is None else jnp.where(group == x, part, mine)
            theirs = None
            for s in range(3):
                shift = (32 * s - slot_shift) % LANES
                part = peer[s, slot_part, rows]
                part = pltpu.roll(part, shift, 1) if shift else part
                theirs = part if theirs is None else jnp.where(lane // 32 == s, part, theirs)
            store(r, jnp.where(low_half, theirs, mine))
            store(ROWS + r, jnp.where(low_half, mine, theirs))

    for f in range(4):

        def store(r, value, f=f):
            gfld[f, r : r + 8] = value

        build_side(lambda x, rows, f=f: fld[f, x, rows], 0, 32 * f, store)

    def store_mask(r, value):
        gmsk[r : r + 8] = value

    build_side(lambda x, rows: msk[x, rows].astype(jnp.float32), 1, 0, store_mask)

    def first_main(x, carry):
        for r in BLOCKS:
            rows = slice(r, r + 8)
            out = first(fld[0, x, rows], fld[1, x, rows], fld[2, x, rows], fld[3, x, rows], msk[x, rows] == 1)
            for q in range(19):
                main_a[q, x, rows] = out[q]
        return carry

    lax.fori_loop(0, LAYERS, first_main, 0)

    def first_side(i, carry):
        base = i * ROWS
        for r in BLOCKS:
            rows = pl.ds(base + r, 8)
            out = first(gfld[0, rows], gfld[1, rows], gfld[2, rows], gfld[3, rows], gmsk[rows] > 0.5)
            for q in range(19):
                side_a[q, rows] = out[q]
        return carry

    lax.fori_loop(0, 2, first_side, 0)

    def pull_main(main, side, x, r):
        f = []
        for q, (cx, cy, cz) in enumerate(VELOCITIES):
            value = main[q, x - cx, r - cy : r - cy + 8]
            if cz == 1:
                edge = pltpu.roll(side[q, r - cy : r - cy + 8], 125 - 8 * (x - cx), 1)
                value = jnp.where(lane == 0, edge, pltpu.roll(value, 1, 1))
            elif cz == -1:
                edge = pltpu.roll(side[q, ROWS + r - cy : ROWS + r - cy + 8], 123 - 8 * (x - cx), 1)
                value = jnp.where(lane == LANES - 1, edge, pltpu.roll(value, LANES - 1, 1))
            f.append(value)
        return f

    def pull_side(side, base, r):
        f = []
        for q, (cx, cy, cz) in enumerate(VELOCITIES):
            value = side[q, pl.ds(base + r - cy, 8)]
            shift = (8 * cx + cz) % LANES
            f.append(pltpu.roll(value, shift, 1) if shift else value)
        return f

    main, side, main_to, side_to = main_a, side_a, main_b, side_b
    for step in range(1, 4):

        def step_main(x, carry, main=main, side=side, main_to=main_to):
            for r in BLOCKS:
                rows = slice(r, r + 8)
                out = collide(pull_main(main, side, x, r), msk[x, rows] == 1)
                for q in range(19):
                    main_to[q, x, rows] = out[q]
            return carry

        def step_side(i, carry, side=side, side_to=side_to):
            base = i * ROWS
            for r in BLOCKS:
                rows = pl.ds(base + r, 8)
                out = collide(pull_side(side, base, r), gmsk[rows] > 0.5)
                for q in range(19):
                    side_to[q, rows] = out[q]
            return carry

        lax.fori_loop(step, LAYERS - step, step_main, 0)
        lax.fori_loop(0, 2, step_side, 0)
        main, side, main_to, side_to = main_to, side_to, main, side

    def last(x, carry):
        for r in INNER:
            rho, mx, my, mz = moments(pull_main(main, side, x, r))
            rows = slice(r - 8, r)
            out_density[x - 4, rows] = rho
            out_momentum[0, x - 4, rows] = mx
            out_momentum[1, x - 4, rows] = my
            out_momentum[2, x - 4, rows] = mz
        return carry

    lax.fori_loop(4, 8, last, 0)

    for c in y_copies + [z_copy] + x_copies + f_copies:
        c.wait_send()


def local(density, velocity, solid_mask):
    shape = density.shape
    f32 = jnp.float32
    dma = pltpu.SemaphoreType.DMA
    return tuple(
        pl.pallas_call(
            kernel,
            out_shape=(jax.ShapeDtypeStruct(shape, f32), jax.ShapeDtypeStruct((3,) + shape, f32)),
            in_specs=[pl.BlockSpec(memory_space=pl.ANY)] * 3,
            out_specs=(pl.BlockSpec(memory_space=pltpu.VMEM), pl.BlockSpec(memory_space=pltpu.VMEM)),
            scratch_shapes=[
                pltpu.VMEM((4, LAYERS, ROWS, LANES), f32),
                pltpu.VMEM((LAYERS, ROWS, LANES), jnp.int32),
                pltpu.VMEM((2, ROWS, LANES), f32),
                pltpu.VMEM((3, 2, ROWS, LANES), f32),
                pltpu.VMEM((4, 2 * ROWS, LANES), f32),
                pltpu.VMEM((2 * ROWS, LANES), f32),
                pltpu.VMEM((19, LAYERS, ROWS, LANES), f32),
                pltpu.VMEM((19, LAYERS, ROWS, LANES), f32),
                pltpu.VMEM((19, 2 * ROWS, LANES), f32),
                pltpu.VMEM((19, 2 * ROWS, LANES), f32),
                dma((3,)),
                dma((4,)),
                dma((4,)),
                dma,
                dma,
                dma((10,)),
                dma((10,)),
                dma((10,)),
                dma((10,)),
            ],
            compiler_params=pltpu.CompilerParams(collective_id=0, has_side_effects=True, vmem_limit_bytes=48 << 20),
        )(density, velocity, solid_mask)
    )


def solution(mesh):
    return jax.shard_map(
        local,
        mesh=mesh,
        in_specs=(P("gx", "gy", "gz"), P(None, "gx", "gy", "gz"), P("gx", "gy", "gz")),
        out_specs=(P("gx", "gy", "gz"), P(None, "gx", "gy", "gz")),
        check_vma=False,
    )
```

```python
import jax
import jax.numpy as jnp
from jax import lax
from jax.experimental import pallas as pl
from jax.experimental.pallas import tpu as pltpu
from jax.sharding import PartitionSpec as P

MESH = pl.DeviceIdType.MESH

VELOCITIES = [
    (0, 0, 0),
    (1, 0, 0),
    (-1, 0, 0),
    (0, 1, 0),
    (0, -1, 0),
    (0, 0, 1),
    (0, 0, -1),
    (1, 1, 0),
    (-1, -1, 0),
    (1, -1, 0),
    (-1, 1, 0),
    (1, 0, 1),
    (-1, 0, -1),
    (1, 0, -1),
    (-1, 0, 1),
    (0, 1, 1),
    (0, -1, -1),
    (0, 1, -1),
    (0, -1, 1),
]
RELAX_RATE = 1.25
W0, W1, W2 = 1.0 / 3.0, 1.0 / 18.0, 1.0 / 36.0

G = 4
LAYERS, ROWS, LANES = 12, 48, 128
BLOCKS = [4 + 8 * j for j in range(5)]
INNER = [8 + 8 * j for j in range(4)]


def moments(f):
    s = [f[2 * k + 1] + f[2 * k + 2] for k in range(9)]
    d = [f[2 * k + 1] - f[2 * k + 2] for k in range(9)]
    rho = f[0] + (((s[0] + s[1]) + (s[2] + s[3])) + ((s[4] + s[5]) + (s[6] + s[7]))) + s[8]
    mx = d[0] + (d[3] + d[4]) + (d[5] + d[6])
    my = d[1] + (d[3] - d[4]) + (d[7] + d[8])
    mz = d[2] + (d[5] - d[6]) + (d[7] - d[8])
    return rho, (mx, my, mz), s, d


def balance(rho, m, u, scale):
    mx, my, mz = m
    ux, uy, uz = u
    xx, yy, zz = mx * ux, my * uy, mz * uz
    base = (scale * W2) * rho - (1.0 / 3.0) * (xx + yy + zz)
    px, py, pz = (scale * W2 * 3.0) * mx, (scale * W2 * 3.0) * my, (scale * W2 * 3.0) * mz
    ax, ay, az = base + xx, base + yy, base + zz
    pairs = [(ax + ax, px + px), (ay + ay, py + py), (az + az, pz + pz)]
    mx2, my2 = mx + mx, my + my
    for even, cross, pa, pb in (
        (ax + yy, mx2 * uy, px, py),
        (ax + zz, mx2 * uz, px, pz),
        (ay + zz, my2 * uz, py, pz),
    ):
        pairs.append((even + cross, pa + pb))
        pairs.append((even - cross, pa - pb))
    return (W0 / W2) * base, pairs


def first(rho, vx, vy, vz, solid):
    sign = jnp.where(solid, -1.0, 1.0)
    m = tuple((rho * sign) * v for v in (vx, vy, vz))
    half = jnp.where(solid, -W2 * 4.5, W2 * 4.5)
    rest, pairs = balance(rho, m, tuple(half * v for v in (vx, vy, vz)), 1.0)
    out = [rest]
    for even, odd in pairs:
        out += [even + odd, even - odd]
    return out


def collide(f, solid):
    rho, m, s, d = moments(f)
    inv = (RELAX_RATE * W2 * 4.5) / rho
    u = tuple(v * inv for v in m)
    rho, *m = (jnp.where(solid, 0.0, v) for v in (rho, *m))
    rest, pairs = balance(rho, m, u, RELAX_RATE)
    keep = 1.0 - RELAX_RATE
    keep_rest = jnp.where(solid, 1.0, keep)
    keep_sum = jnp.where(solid, 0.5, 0.5 * keep)
    keep_diff = jnp.where(solid, -0.5, 0.5 * keep)
    out = [keep_rest * f[0] + rest]
    for k, (even, odd) in enumerate(pairs):
        even = even + keep_sum * s[k]
        odd = odd + keep_diff * d[k]
        out += [even + odd, even - odd]
    return out


def kernel(
    density,
    velocity,
    mask,
    out_density,
    out_momentum,
    fld,
    msk,
    pack,
    peer,
    gfld,
    gmsk,
    main_a,
    main_b,
    side_a,
    side_b,
    load_sem,
    y_send,
    y_recv,
    z_send,
    z_recv,
    x_send,
    x_recv,
    f_send,
    f_recv,
):
    gx, gy, gz = lax.axis_index("gx"), lax.axis_index("gy"), lax.axis_index("gz")
    par = lax.rem(gx, 2)
    y_up = (gx, lax.rem(gy + 1, 8), gz)
    y_down = (gx, lax.rem(gy + 7, 8), gz)
    z_peer = (gx, gy, 1 - gz)
    x_peer = (gx + 1 - 2 * par, gy, gz)
    fwd_to = (lax.rem(gx + 2 + 4 * par, 8), gy, gz)
    fwd_from = (lax.rem(gx + 6 - 4 * par, 8), gy, gz)

    loads = [
        pltpu.make_async_copy(density, fld.at[0, 4:8, 8:40], load_sem.at[0]),
        pltpu.make_async_copy(velocity, fld.at[1:4, 4:8, 8:40], load_sem.at[1]),
        pltpu.make_async_copy(mask, msk.at[4:8, 8:40], load_sem.at[2]),
    ]
    for c in loads:
        c.start()

    barrier = pltpu.get_barrier_semaphore()
    for dev in (y_up, y_down, z_peer, x_peer, fwd_to, fwd_from):
        pl.semaphore_signal(barrier, inc=1, device_id=dev, device_id_type=MESH)
    pl.semaphore_wait(barrier, 6)
    for c in loads:
        c.wait()

    def remote(src, dst, send, recv, dev):
        return pltpu.make_async_remote_copy(
            src_ref=src, dst_ref=dst, send_sem=send, recv_sem=recv, device_id=dev, device_id_type=MESH
        )

    y_copies = [
        remote(fld.at[:, 4:8, 36:40], fld.at[:, 4:8, 4:8], y_send.at[0], y_recv.at[0], y_up),
        remote(fld.at[:, 4:8, 8:12], fld.at[:, 4:8, 40:44], y_send.at[1], y_recv.at[1], y_down),
        remote(msk.at[4:8, 36:40], msk.at[4:8, 4:8], y_send.at[2], y_recv.at[2], y_up),
        remote(msk.at[4:8, 8:12], msk.at[4:8, 40:44], y_send.at[3], y_recv.at[3], y_down),
    ]
    for c in y_copies:
        c.start()

    near = pl.ds(8 * (1 - par), 4)
    far = pl.ds(8 * par, 4)
    near_slot, far_slot = 2 * (1 - par), 2 * par

    def parts(layers, slot):
        refs = [fld.at[f, layers, 8:40] for f in range(4)] + [msk.at[layers, 8:40]]
        refs += [fld.at[:, layers, 4:8], fld.at[:, layers, 40:44], msk.at[layers, 4:8], msk.at[layers, 40:44]]
        refs += [peer.at[slot, :, 4:44]]
        return refs

    own = pl.ds(4, 4)
    x_copies = [
        remote(a, b, x_send.at[i], x_recv.at[i], x_peer)
        for i, (a, b) in enumerate(zip(parts(own, 1), parts(far, far_slot)))
    ]
    f_copies = [
        remote(a, b, f_send.at[i], f_recv.at[i], fwd_to)
        for i, (a, b) in enumerate(zip(parts(near, near_slot), parts(far, far_slot)))
    ]
    for c in x_copies[:5]:
        c.start()
    for c in y_copies:
        c.wait_recv()
    for c in x_copies[5:9]:
        c.start()

    lane = lax.broadcasted_iota(jnp.int32, (8, LANES), 1)
    group = lane // 8
    low_half = lax.rem(lane, 8) < 4

    for r in BLOCKS:
        rows = slice(r, r + 8)
        acc = None
        for f in range(4):
            for x in range(4):
                part = pltpu.roll(fld[f, 4 + x, rows], 32 * f + 8 * x + 4, 1)
                acc = part if acc is None else jnp.where(group == 4 * f + x, part, acc)
        pack[0, rows] = acc
        acc = None
        for x in range(4):
            part = pltpu.roll(msk[4 + x, rows].astype(jnp.float32), 8 * x + 4, 1)
            acc = part if acc is None else jnp.where(group == x, part, acc)
        pack[1, rows] = acc

    def first_layer(x):
        for r in BLOCKS:
            rows = slice(r, r + 8)
            out = first(fld[0, x, rows], fld[1, x, rows], fld[2, x, rows], fld[3, x, rows], msk[x, rows] == 1)
            for q in range(19):
                main_a[q, x, rows] = out[q]

    def first_four(start):
        def body(i, carry):
            first_layer(start + 2 * i)
            first_layer(start + 2 * i + 1)
            return carry

        lax.fori_loop(0, 2, body, 0)

    def first_side():
        def body(i, carry):
            for r in BLOCKS:
                rows = pl.ds(i * ROWS + r, 8)
                out = first(gfld[0, rows], gfld[1, rows], gfld[2, rows], gfld[3, rows], gmsk[rows] > 0.5)
                for q in range(19):
                    side_a[q, rows] = out[q]
            return carry

        lax.fori_loop(0, 2, body, 0)

    def build_side(start, count, slots, fresh):
        for f in range(5):
            shift_back = 32 * f if f < 4 else 0
            for r in BLOCKS:
                rows = slice(r, r + 8)
                low, high = slice(r, r + 8), slice(ROWS + r, ROWS + r + 8)
                mine = theirs = None
                for i in range(count):
                    x = start + i
                    part = fld[f, x, rows] if f < 4 else msk[x, rows].astype(jnp.float32)
                    part = pltpu.roll(part, lax.rem(8 * x + 4, LANES), 1)
                    mine = part if mine is None else jnp.where(group == x, part, mine)
                for s in slots:
                    part = peer[s, f // 4, rows]
                    part = pltpu.roll(part, lax.rem(32 * s + LANES - shift_back, LANES), 1)
                    theirs = part if theirs is None else jnp.where(lane // 32 == s, part, theirs)
                below = jnp.where(low_half, theirs, mine)
                above = jnp.where(low_half, mine, theirs)
                if not fresh:
                    here = lane // 32 == slots[0]
                    old = (gfld[f, low], gfld[f, high]) if f < 4 else (gmsk[low], gmsk[high])
                    below, above = jnp.where(here, below, old[0]), jnp.where(here, above, old[1])
                if f < 4:
                    gfld[f, low] = below
                    gfld[f, high] = above
                else:
                    gmsk[low] = below
                    gmsk[high] = above

    def pull_main(main, side, x, r):
        f = []
        for q, (cx, cy, cz) in enumerate(VELOCITIES):
            value = main[q, x - cx, r - cy : r - cy + 8]
            if cz == 1:
                edge = pltpu.roll(side[q, r - cy : r - cy + 8], 125 - 8 * (x - cx), 1)
                value = jnp.where(lane == 0, edge, pltpu.roll(value, 1, 1))
            elif cz == -1:
                edge = pltpu.roll(side[q, ROWS + r - cy : ROWS + r - cy + 8], 123 - 8 * (x - cx), 1)
                value = jnp.where(lane == LANES - 1, edge, pltpu.roll(value, LANES - 1, 1))
            f.append(value)
        return f

    def pull_side(side, base, r):
        f = []
        for q, (cx, cy, cz) in enumerate(VELOCITIES):
            value = side[q, pl.ds(base + r - cy, 8)]
            shift = (8 * cx + cz) % LANES
            f.append(pltpu.roll(value, shift, 1) if shift else value)
        return f

    buffers = [(main_a, side_a), (main_b, side_b)]

    def step_layers(step, start, count):
        (main, side), (main_to, _) = buffers[step % 2], buffers[(step + 1) % 2]

        def body(i, carry):
            for k in range(2):
                x = start + 2 * i + k
                for r in BLOCKS:
                    rows = slice(r, r + 8)
                    out = collide(pull_main(main, side, x, r), msk[x, rows] == 1)
                    for q in range(19):
                        main_to[q, x, rows] = out[q]
            return carry

        lax.fori_loop(0, count // 2, body, 0)

    def step_side(step):
        (_, side), (_, side_to) = buffers[step % 2], buffers[(step + 1) % 2]

        def body(i, carry):
            for r in BLOCKS:
                rows = pl.ds(i * ROWS + r, 8)
                out = collide(pull_side(side, i * ROWS, r), gmsk[rows] > 0.5)
                for q in range(19):
                    side_to[q, rows] = out[q]
            return carry

        lax.fori_loop(0, 2, body, 0)

    first_four(4)
    z_copy = remote(pack.at[:, 4:44], peer.at[1, :, 4:44], z_send, z_recv, z_peer)
    z_copy.start()
    x_copies[0].wait_recv()
    f_copies[0].start()
    x_copies[1].wait_recv()
    f_copies[1].start()
    z_copy.wait_recv()
    x_copies[9].start()
    for i in range(2, 10):
        x_copies[i].wait_recv()
        f_copies[i].start()

    build_side(4 - 4 * par, 8, (1 - par, 2 - par), True)
    first_four(8 - 8 * par)
    first_side()
    step_layers(2, 5 - 4 * par, 6)
    step_side(2)
    step_layers(3, 6 - 4 * par, 4)
    step_side(3)
    step_layers(4, 7 - 4 * par, 2)

    for c in f_copies:
        c.wait_recv()
    build_side(8 * par, 4, (2 * par,), False)
    first_four(8 * par)
    first_side()
    step_layers(2, 1 + 6 * par, 4)
    step_side(2)
    step_layers(3, 2 + 4 * par, 4)
    step_side(3)
    step_layers(4, 3 + 2 * par, 4)
    step_side(4)

    def last(x, carry):
        for r in INNER:
            rho, m, _, _ = moments(pull_main(main_b, side_b, x, r))
            rows = slice(r - 8, r)
            out_density[x - 4, rows] = rho
            for k in range(3):
                out_momentum[k, x - 4, rows] = m[k]
        return carry

    lax.fori_loop(4, 8, last, 0)

    for c in y_copies + [z_copy] + x_copies + f_copies:
        c.wait_send()


def local(density, velocity, solid_mask):
    shape = density.shape
    f32 = jnp.float32
    dma = pltpu.SemaphoreType.DMA
    return tuple(
        pl.pallas_call(
            kernel,
            out_shape=(jax.ShapeDtypeStruct(shape, f32), jax.ShapeDtypeStruct((3,) + shape, f32)),
            in_specs=[pl.BlockSpec(memory_space=pl.ANY)] * 3,
            out_specs=(pl.BlockSpec(memory_space=pltpu.VMEM), pl.BlockSpec(memory_space=pltpu.VMEM)),
            scratch_shapes=[
                pltpu.VMEM((4, LAYERS, ROWS, LANES), f32),
                pltpu.VMEM((LAYERS, ROWS, LANES), jnp.int32),
                pltpu.VMEM((2, ROWS, LANES), f32),
                pltpu.VMEM((3, 2, ROWS, LANES), f32),
                pltpu.VMEM((4, 2 * ROWS, LANES), f32),
                pltpu.VMEM((2 * ROWS, LANES), f32),
                pltpu.VMEM((19, LAYERS, ROWS, LANES), f32),
                pltpu.VMEM((19, LAYERS, ROWS, LANES), f32),
                pltpu.VMEM((19, 2 * ROWS, LANES), f32),
                pltpu.VMEM((19, 2 * ROWS, LANES), f32),
                dma((3,)),
                dma((4,)),
                dma((4,)),
                dma,
                dma,
                dma((10,)),
                dma((10,)),
                dma((10,)),
                dma((10,)),
            ],
            compiler_params=pltpu.CompilerParams(collective_id=0, has_side_effects=True, vmem_limit_bytes=67043328),
        )(density, velocity, solid_mask)
    )


def solution(mesh):
    return jax.shard_map(
        local,
        mesh=mesh,
        in_specs=(P("gx", "gy", "gz"), P(None, "gx", "gy", "gz"), P("gx", "gy", "gz")),
        out_specs=(P("gx", "gy", "gz"), P(None, "gx", "gy", "gz")),
        check_vma=False,
    )
```

```python
import jax
import jax.numpy as jnp
from jax import lax
from jax.experimental import pallas as pl
from jax.experimental.pallas import tpu as pltpu
from jax.sharding import PartitionSpec as P

MESH = pl.DeviceIdType.MESH

VELOCITIES = [
    (0, 0, 0),
    (1, 0, 0),
    (-1, 0, 0),
    (0, 1, 0),
    (0, -1, 0),
    (0, 0, 1),
    (0, 0, -1),
    (1, 1, 0),
    (-1, -1, 0),
    (1, -1, 0),
    (-1, 1, 0),
    (1, 0, 1),
    (-1, 0, -1),
    (1, 0, -1),
    (-1, 0, 1),
    (0, 1, 1),
    (0, -1, -1),
    (0, 1, -1),
    (0, -1, 1),
]
RELAX_RATE = 1.25
W0, W1, W2 = 1.0 / 3.0, 1.0 / 18.0, 1.0 / 36.0

G = 4
LAYERS, ROWS, LANES = 12, 48, 128
BLOCKS = [4 + 8 * j for j in range(5)]
INNER = [8 + 8 * j for j in range(4)]


def moments(f):
    s = [f[2 * k + 1] + f[2 * k + 2] for k in range(9)]
    d = [f[2 * k + 1] - f[2 * k + 2] for k in range(9)]
    rho = f[0] + (((s[0] + s[1]) + (s[2] + s[3])) + ((s[4] + s[5]) + (s[6] + s[7]))) + s[8]
    mx = d[0] + (d[3] + d[4]) + (d[5] + d[6])
    my = d[1] + (d[3] - d[4]) + (d[7] + d[8])
    mz = d[2] + (d[5] - d[6]) + (d[7] - d[8])
    return rho, (mx, my, mz), s, d


def balance(rho, m, u, scale):
    mx, my, mz = m
    ux, uy, uz = u
    xx, yy, zz = mx * ux, my * uy, mz * uz
    base = (scale * W2) * rho - (1.0 / 3.0) * (xx + yy + zz)
    px, py, pz = (scale * W2 * 3.0) * mx, (scale * W2 * 3.0) * my, (scale * W2 * 3.0) * mz
    ax, ay, az = base + xx, base + yy, base + zz
    pairs = [(ax + ax, px + px), (ay + ay, py + py), (az + az, pz + pz)]
    mx2, my2 = mx + mx, my + my
    for even, cross, pa, pb in (
        (ax + yy, mx2 * uy, px, py),
        (ax + zz, mx2 * uz, px, pz),
        (ay + zz, my2 * uz, py, pz),
    ):
        pairs.append((even + cross, pa + pb))
        pairs.append((even - cross, pa - pb))
    return (W0 / W2) * base, pairs


def first(rho, vx, vy, vz, solid):
    sign = jnp.where(solid, -1.0, 1.0)
    m = tuple((rho * sign) * v for v in (vx, vy, vz))
    half = jnp.where(solid, -W2 * 4.5, W2 * 4.5)
    rest, pairs = balance(rho, m, tuple(half * v for v in (vx, vy, vz)), 1.0)
    out = [rest]
    for even, odd in pairs:
        out += [even + odd, even - odd]
    return out


def collide(f, solid):
    rho, m, s, d = moments(f)
    inv = (RELAX_RATE * W2 * 4.5) / rho
    u = tuple(v * inv for v in m)
    rho, *m = (jnp.where(solid, 0.0, v) for v in (rho, *m))
    rest, pairs = balance(rho, m, u, RELAX_RATE)
    keep = 1.0 - RELAX_RATE
    keep_rest = jnp.where(solid, 1.0, keep)
    keep_sum = jnp.where(solid, 0.5, 0.5 * keep)
    keep_diff = jnp.where(solid, -0.5, 0.5 * keep)
    out = [keep_rest * f[0] + rest]
    for k, (even, odd) in enumerate(pairs):
        even = even + keep_sum * s[k]
        odd = odd + keep_diff * d[k]
        out += [even + odd, even - odd]
    return out


def kernel(
    density,
    velocity,
    mask,
    out,
    fld,
    msk,
    pack,
    peer,
    gfld,
    gmsk,
    main_a,
    main_b,
    side_a,
    side_b,
    load_sem,
    y_send,
    y_recv,
    z_send,
    z_recv,
    x_send,
    x_recv,
    f_send,
    f_recv,
):
    gx, gy, gz = lax.axis_index("gx"), lax.axis_index("gy"), lax.axis_index("gz")
    par = lax.rem(gx, 2)
    y_up = (gx, lax.rem(gy + 1, 8), gz)
    y_down = (gx, lax.rem(gy + 7, 8), gz)
    z_peer = (gx, gy, 1 - gz)
    x_peer = (gx + 1 - 2 * par, gy, gz)
    fwd_to = (lax.rem(gx + 2 + 4 * par, 8), gy, gz)
    fwd_from = (lax.rem(gx + 6 - 4 * par, 8), gy, gz)

    loads = [
        pltpu.make_async_copy(density, fld.at[0, 4:8, 8:40], load_sem.at[0]),
        pltpu.make_async_copy(velocity, fld.at[1:4, 4:8, 8:40], load_sem.at[1]),
        pltpu.make_async_copy(mask, msk.at[4:8, 8:40], load_sem.at[2]),
    ]
    for c in loads:
        c.start()

    barrier = pltpu.get_barrier_semaphore()
    for dev in (y_up, y_down, z_peer, x_peer, fwd_to, fwd_from):
        pl.semaphore_signal(barrier, inc=1, device_id=dev, device_id_type=MESH)

    lane = lax.broadcasted_iota(jnp.int32, (8, LANES), 1)
    group = lane // 8
    low_half = lax.rem(lane, 8) < 4

    def pack_rows(r):
        rows = slice(r, r + 8)
        acc = None
        for f in range(4):
            for x in range(4):
                part = pltpu.roll(fld[f, 4 + x, rows], 32 * f + 8 * x + 4, 1)
                acc = part if acc is None else jnp.where(group == 4 * f + x, part, acc)
        pack[0, rows] = acc
        acc = None
        for x in range(4):
            part = pltpu.roll(msk[4 + x, rows].astype(jnp.float32), 8 * x + 4, 1)
            acc = part if acc is None else jnp.where(group == x, part, acc)
        pack[1, rows] = acc

    for c in loads:
        c.wait()
    for r in BLOCKS[1:-1]:
        pack_rows(r)
    pl.semaphore_wait(barrier, 6)

    def remote(src, dst, send, recv, dev):
        return pltpu.make_async_remote_copy(
            src_ref=src, dst_ref=dst, send_sem=send, recv_sem=recv, device_id=dev, device_id_type=MESH
        )

    y_copies = [
        remote(fld.at[:, 4:8, 36:40], fld.at[:, 4:8, 4:8], y_send.at[0], y_recv.at[0], y_up),
        remote(fld.at[:, 4:8, 8:12], fld.at[:, 4:8, 40:44], y_send.at[1], y_recv.at[1], y_down),
        remote(msk.at[4:8, 36:40], msk.at[4:8, 4:8], y_send.at[2], y_recv.at[2], y_up),
        remote(msk.at[4:8, 8:12], msk.at[4:8, 40:44], y_send.at[3], y_recv.at[3], y_down),
    ]
    for c in y_copies:
        c.start()

    near = pl.ds(8 * (1 - par), 4)
    far = pl.ds(8 * par, 4)
    near_slot, far_slot = 2 * (1 - par), 2 * par

    def parts(layers, slot):
        refs = [fld.at[f, layers, 8:40] for f in range(4)] + [msk.at[layers, 8:40]]
        refs += [fld.at[:, layers, 4:8], fld.at[:, layers, 40:44], msk.at[layers, 4:8], msk.at[layers, 40:44]]
        refs += [peer.at[slot, :, 4:44]]
        return refs

    own = pl.ds(4, 4)
    x_copies = [
        remote(a, b, x_send.at[i], x_recv.at[i], x_peer)
        for i, (a, b) in enumerate(zip(parts(own, 1), parts(far, far_slot)))
    ]
    f_copies = [
        remote(a, b, f_send.at[i], f_recv.at[i], fwd_to)
        for i, (a, b) in enumerate(zip(parts(near, near_slot), parts(far, far_slot)))
    ]
    for c in x_copies[:4]:
        c.start()
    for c in y_copies:
        c.wait_recv()
    pack_rows(BLOCKS[0])
    pack_rows(BLOCKS[-1])

    def first_layer(x):
        for r in BLOCKS:
            rows = slice(r, r + 8)
            out = first(fld[0, x, rows], fld[1, x, rows], fld[2, x, rows], fld[3, x, rows], msk[x, rows] == 1)
            for q in range(19):
                main_a[q, x, rows] = out[q]

    def first_four(start):
        def body(i, carry):
            first_layer(start + 2 * i)
            first_layer(start + 2 * i + 1)
            return carry

        lax.fori_loop(0, 2, body, 0)

    def first_side():
        def body(i, carry):
            for r in BLOCKS:
                rows = pl.ds(i * ROWS + r, 8)
                out = first(gfld[0, rows], gfld[1, rows], gfld[2, rows], gfld[3, rows], gmsk[rows] > 0.5)
                for q in range(19):
                    side_a[q, rows] = out[q]
            return carry

        lax.fori_loop(0, 2, body, 0)

    def build_side(start, count, slots, fresh):
        for f in range(5):
            shift_back = 32 * f if f < 4 else 0
            for r in BLOCKS:
                rows = slice(r, r + 8)
                low, high = slice(r, r + 8), slice(ROWS + r, ROWS + r + 8)
                mine = theirs = None
                for i in range(count):
                    x = start + i
                    part = fld[f, x, rows] if f < 4 else msk[x, rows].astype(jnp.float32)
                    part = pltpu.roll(part, lax.rem(8 * x + 4, LANES), 1)
                    mine = part if mine is None else jnp.where(group == x, part, mine)
                for s in slots:
                    part = peer[s, f // 4, rows]
                    part = pltpu.roll(part, lax.rem(32 * s + LANES - shift_back, LANES), 1)
                    theirs = part if theirs is None else jnp.where(lane // 32 == s, part, theirs)
                below = jnp.where(low_half, theirs, mine)
                above = jnp.where(low_half, mine, theirs)
                if not fresh:
                    here = lane // 32 == slots[0]
                    old = (gfld[f, low], gfld[f, high]) if f < 4 else (gmsk[low], gmsk[high])
                    below, above = jnp.where(here, below, old[0]), jnp.where(here, above, old[1])
                if f < 4:
                    gfld[f, low] = below
                    gfld[f, high] = above
                else:
                    gmsk[low] = below
                    gmsk[high] = above

    def pull_main(main, side, x, r):
        f = []
        for q, (cx, cy, cz) in enumerate(VELOCITIES):
            value = main[q, x - cx, r - cy : r - cy + 8]
            if cz == 1:
                edge = pltpu.roll(side[q, r - cy : r - cy + 8], 125 - 8 * (x - cx), 1)
                value = jnp.where(lane == 0, edge, pltpu.roll(value, 1, 1))
            elif cz == -1:
                edge = pltpu.roll(side[q, ROWS + r - cy : ROWS + r - cy + 8], 123 - 8 * (x - cx), 1)
                value = jnp.where(lane == LANES - 1, edge, pltpu.roll(value, LANES - 1, 1))
            f.append(value)
        return f

    def pull_side(side, base, r):
        f = []
        for q, (cx, cy, cz) in enumerate(VELOCITIES):
            value = side[q, pl.ds(base + r - cy, 8)]
            shift = (8 * cx + cz) % LANES
            f.append(pltpu.roll(value, shift, 1) if shift else value)
        return f

    buffers = [(main_a, side_a), (main_b, side_b)]

    def step_layers(step, start, count):
        (main, side), (main_to, _) = buffers[step % 2], buffers[(step + 1) % 2]

        def body(i, carry):
            for k in range(2):
                x = start + 2 * i + k
                for r in BLOCKS:
                    rows = slice(r, r + 8)
                    out = collide(pull_main(main, side, x, r), msk[x, rows] == 1)
                    for q in range(19):
                        main_to[q, x, rows] = out[q]
            return carry

        lax.fori_loop(0, count // 2, body, 0)

    def step_side(step):
        (_, side), (_, side_to) = buffers[step % 2], buffers[(step + 1) % 2]

        def body(i, carry):
            for r in BLOCKS:
                rows = pl.ds(i * ROWS + r, 8)
                out = collide(pull_side(side, i * ROWS, r), gmsk[rows] > 0.5)
                for q in range(19):
                    side_to[q, rows] = out[q]
            return carry

        lax.fori_loop(0, 2, body, 0)

    first_four(4)
    z_copy = remote(pack.at[:, 4:44], peer.at[1, :, 4:44], z_send, z_recv, z_peer)
    z_copy.start()
    for c in x_copies[4:9]:
        c.start()
    x_copies[0].wait_recv()
    f_copies[0].start()
    for i in range(1, 4):
        x_copies[i].wait_recv()
        f_copies[i].start()
    z_copy.wait_recv()
    x_copies[9].start()
    for i in range(4, 10):
        x_copies[i].wait_recv()
        f_copies[i].start()

    build_side(4 - 4 * par, 8, (1 - par, 2 - par), True)
    first_four(8 - 8 * par)
    first_side()
    step_layers(2, 5 - 4 * par, 6)
    step_side(2)
    step_layers(3, 6 - 4 * par, 4)
    step_side(3)
    step_layers(4, 7 - 4 * par, 2)

    for c in f_copies:
        c.wait_recv()
    build_side(8 * par, 4, (2 * par,), False)
    first_four(8 * par)
    first_side()
    step_layers(2, 1 + 6 * par, 4)
    step_side(2)
    step_layers(3, 2 + 4 * par, 4)
    step_side(3)
    step_layers(4, 3 + 2 * par, 4)
    step_side(4)

    def last(x, carry):
        for r in INNER:
            rho, m, _, _ = moments(pull_main(main_b, side_b, x, r))
            rows = slice(r - 8, r)
            for k, value in enumerate((rho, *m)):
                out[k, x - 4, rows] = value
        return carry

    lax.fori_loop(4, 8, last, 0)

    for c in y_copies + [z_copy] + x_copies + f_copies:
        c.wait_send()


def split(both, density, momentum, sem):
    copies = [
        pltpu.make_async_copy(both.at[0], density, sem.at[0]),
        pltpu.make_async_copy(both.at[1:4], momentum, sem.at[1]),
    ]
    for c in copies:
        c.start()
    for c in copies:
        c.wait()


def local(density, velocity, solid_mask):
    shape = density.shape
    f32 = jnp.float32
    dma = pltpu.SemaphoreType.DMA
    both = pl.pallas_call(
            kernel,
            out_shape=jax.ShapeDtypeStruct((4,) + shape, f32),
            in_specs=[pl.BlockSpec(memory_space=pl.ANY)] * 3,
            out_specs=pl.BlockSpec(memory_space=pltpu.VMEM),
            scratch_shapes=[
                pltpu.VMEM((4, LAYERS, ROWS, LANES), f32),
                pltpu.VMEM((LAYERS, ROWS, LANES), jnp.int32),
                pltpu.VMEM((2, ROWS, LANES), f32),
                pltpu.VMEM((3, 2, ROWS, LANES), f32),
                pltpu.VMEM((4, 2 * ROWS, LANES), f32),
                pltpu.VMEM((2 * ROWS, LANES), f32),
                pltpu.VMEM((19, LAYERS, ROWS, LANES), f32),
                pltpu.VMEM((19, LAYERS, ROWS, LANES), f32),
                pltpu.VMEM((19, 2 * ROWS, LANES), f32),
                pltpu.VMEM((19, 2 * ROWS, LANES), f32),
                dma((3,)),
                dma((4,)),
                dma((4,)),
                dma,
                dma,
                dma((10,)),
                dma((10,)),
                dma((10,)),
                dma((10,)),
            ],
            compiler_params=pltpu.CompilerParams(collective_id=0, has_side_effects=True, vmem_limit_bytes=51043328),
        )(*[pltpu.with_memory_space_constraint(v, pltpu.HBM) for v in (density, velocity, solid_mask)])
    return tuple(
        pl.pallas_call(
            split,
            out_shape=(jax.ShapeDtypeStruct(shape, f32), jax.ShapeDtypeStruct((3,) + shape, f32)),
            in_specs=[pl.BlockSpec(memory_space=pltpu.VMEM)],
            out_specs=(pl.BlockSpec(memory_space=pl.ANY), pl.BlockSpec(memory_space=pl.ANY)),
            scratch_shapes=[dma((2,))],
            compiler_params=pltpu.CompilerParams(vmem_limit_bytes=32 << 20),
        )(both)
    )


def solution(mesh):
    return jax.shard_map(
        local,
        mesh=mesh,
        in_specs=(P("gx", "gy", "gz"), P(None, "gx", "gy", "gz"), P("gx", "gy", "gz")),
        out_specs=(P("gx", "gy", "gz"), P(None, "gx", "gy", "gz")),
        check_vma=False,
    )
```

```python
import jax
import jax.numpy as jnp
from jax import lax
from jax.experimental import pallas as pl
from jax.experimental.pallas import tpu as pltpu
from jax.sharding import PartitionSpec as P

MESH = pl.DeviceIdType.MESH

VELOCITIES = [
    (0, 0, 0),
    (1, 0, 0),
    (-1, 0, 0),
    (0, 1, 0),
    (0, -1, 0),
    (0, 0, 1),
    (0, 0, -1),
    (1, 1, 0),
    (-1, -1, 0),
    (1, -1, 0),
    (-1, 1, 0),
    (1, 0, 1),
    (-1, 0, -1),
    (1, 0, -1),
    (-1, 0, 1),
    (0, 1, 1),
    (0, -1, -1),
    (0, 1, -1),
    (0, -1, 1),
]
RELAX_RATE = 1.25
W0, W1, W2 = 1.0 / 3.0, 1.0 / 18.0, 1.0 / 36.0

G = 4
LAYERS, ROWS, LANES = 12, 48, 128
BLOCKS = [4 + 8 * j for j in range(5)]
INNER = [8 + 8 * j for j in range(4)]


def moments(f):
    s = [f[2 * k + 1] + f[2 * k + 2] for k in range(9)]
    d = [f[2 * k + 1] - f[2 * k + 2] for k in range(9)]
    rho = f[0] + (((s[0] + s[1]) + (s[2] + s[3])) + ((s[4] + s[5]) + (s[6] + s[7]))) + s[8]
    mx = d[0] + (d[3] + d[4]) + (d[5] + d[6])
    my = d[1] + (d[3] - d[4]) + (d[7] + d[8])
    mz = d[2] + (d[5] - d[6]) + (d[7] - d[8])
    return rho, (mx, my, mz), s, d


def balance(rho, m, u, scale):
    mx, my, mz = m
    ux, uy, uz = u
    xx, yy, zz = mx * ux, my * uy, mz * uz
    base = (scale * W2) * rho - (1.0 / 3.0) * (xx + yy + zz)
    px, py, pz = (scale * W2 * 3.0) * mx, (scale * W2 * 3.0) * my, (scale * W2 * 3.0) * mz
    ax, ay, az = base + xx, base + yy, base + zz
    pairs = [(ax + ax, px + px), (ay + ay, py + py), (az + az, pz + pz)]
    mx2, my2 = mx + mx, my + my
    for even, cross, pa, pb in (
        (ax + yy, mx2 * uy, px, py),
        (ax + zz, mx2 * uz, px, pz),
        (ay + zz, my2 * uz, py, pz),
    ):
        pairs.append((even + cross, pa + pb))
        pairs.append((even - cross, pa - pb))
    return (W0 / W2) * base, pairs


def first(rho, vx, vy, vz, solid):
    sign = jnp.where(solid, -1.0, 1.0)
    m = tuple((rho * sign) * v for v in (vx, vy, vz))
    half = jnp.where(solid, -W2 * 4.5, W2 * 4.5)
    rest, pairs = balance(rho, m, tuple(half * v for v in (vx, vy, vz)), 1.0)
    out = [rest]
    for even, odd in pairs:
        out += [even + odd, even - odd]
    return out


def collide(f, solid):
    rho, m, s, d = moments(f)
    inv = (RELAX_RATE * W2 * 4.5) / rho
    u = tuple(v * inv for v in m)
    rho, *m = (jnp.where(solid, 0.0, v) for v in (rho, *m))
    rest, pairs = balance(rho, m, u, RELAX_RATE)
    keep = 1.0 - RELAX_RATE
    keep_rest = jnp.where(solid, 1.0, keep)
    keep_sum = jnp.where(solid, 0.5, 0.5 * keep)
    keep_diff = jnp.where(solid, -0.5, 0.5 * keep)
    out = [keep_rest * f[0] + rest]
    for k, (even, odd) in enumerate(pairs):
        even = even + keep_sum * s[k]
        odd = odd + keep_diff * d[k]
        out += [even + odd, even - odd]
    return out


def kernel(
    density,
    velocity,
    mask,
    out,
    fld,
    msk,
    pack,
    peer,
    gfld,
    gmsk,
    main_a,
    main_b,
    side_a,
    side_b,
    load_sem,
    y_send,
    y_recv,
    z_send,
    z_recv,
    x_send,
    x_recv,
    f_send,
    f_recv,
    e_send,
    e_recv,
):
    gx, gy, gz = lax.axis_index("gx"), lax.axis_index("gy"), lax.axis_index("gz")
    par = lax.rem(gx, 2)
    y_up = (gx, lax.rem(gy + 1, 8), gz)
    y_down = (gx, lax.rem(gy + 7, 8), gz)
    z_peer = (gx, gy, 1 - gz)
    x_peer = (gx + 1 - 2 * par, gy, gz)
    fwd_to = (lax.rem(gx + 2 + 4 * par, 8), gy, gz)
    fwd_from = (lax.rem(gx + 6 - 4 * par, 8), gy, gz)

    loads = [
        pltpu.make_async_copy(density, fld.at[0, 4:8, 8:40], load_sem.at[0]),
        pltpu.make_async_copy(velocity, fld.at[1:4, 4:8, 8:40], load_sem.at[1]),
        pltpu.make_async_copy(mask, msk.at[4:8, 8:40], load_sem.at[2]),
    ]
    for c in loads:
        c.start()

    barrier = pltpu.get_barrier_semaphore()
    for dev in (y_up, y_down, z_peer, x_peer, fwd_to, fwd_from):
        pl.semaphore_signal(barrier, inc=1, device_id=dev, device_id_type=MESH)

    lane = lax.broadcasted_iota(jnp.int32, (8, LANES), 1)
    group = lane // 8
    low_half = lax.rem(lane, 8) < 4

    def pack_rows(r):
        rows = slice(r, r + 8)
        acc = None
        for f in range(4):
            for x in range(4):
                part = pltpu.roll(fld[f, 4 + x, rows], 32 * f + 8 * x + 4, 1)
                acc = part if acc is None else jnp.where(group == 4 * f + x, part, acc)
        pack[0, rows] = acc
        acc = None
        for x in range(4):
            part = pltpu.roll(msk[4 + x, rows].astype(jnp.float32), 8 * x + 4, 1)
            acc = part if acc is None else jnp.where(group == x, part, acc)
        pack[1, rows] = acc

    for c in loads:
        c.wait()
    for r in BLOCKS[1:-1]:
        pack_rows(r)
    pl.semaphore_wait(barrier, 6)

    def remote(src, dst, send, recv, dev):
        return pltpu.make_async_remote_copy(
            src_ref=src, dst_ref=dst, send_sem=send, recv_sem=recv, device_id=dev, device_id_type=MESH
        )

    y_copies = [
        remote(fld.at[:, 4:8, 36:40], fld.at[:, 4:8, 4:8], y_send.at[0], y_recv.at[0], y_up),
        remote(fld.at[:, 4:8, 8:12], fld.at[:, 4:8, 40:44], y_send.at[1], y_recv.at[1], y_down),
        remote(msk.at[4:8, 36:40], msk.at[4:8, 4:8], y_send.at[2], y_recv.at[2], y_up),
        remote(msk.at[4:8, 8:12], msk.at[4:8, 40:44], y_send.at[3], y_recv.at[3], y_down),
    ]
    for c in y_copies:
        c.start()

    near = pl.ds(8 * (1 - par), 4)
    far = pl.ds(8 * par, 4)
    near_slot, far_slot = 2 * (1 - par), 2 * par

    def parts(layers, slot):
        refs = [fld.at[f, layers, 8:40] for f in range(4)] + [msk.at[layers, 8:40]]
        refs += [fld.at[3, layers, 4:8], fld.at[3, layers, 40:44], msk.at[layers, 4:8], msk.at[layers, 40:44]]
        refs += [peer.at[slot, :, 4:44]]
        return refs

    own = pl.ds(4, 4)
    x_copies = [
        remote(a, b, x_send.at[i], x_recv.at[i], x_peer)
        for i, (a, b) in enumerate(zip(parts(own, 1), parts(far, far_slot)))
    ]
    f_copies = [
        remote(a, b, f_send.at[i], f_recv.at[i], fwd_to)
        for i, (a, b) in enumerate(zip(parts(near, near_slot), parts(far, far_slot)))
    ]
    e_copies = []
    for i, layers in enumerate((near, far)):
        up, down = fld.at[0:3, layers, 36:40], fld.at[0:3, layers, 8:12]
        e_copies += [
            remote(up, fld.at[0:3, layers, 4:8], e_send.at[2 * i], e_recv.at[2 * i], y_up),
            remote(down, fld.at[0:3, layers, 40:44], e_send.at[2 * i + 1], e_recv.at[2 * i + 1], y_down),
        ]
    for c in x_copies[:3]:
        c.start()
    for c in y_copies:
        c.wait_recv()
    pack_rows(BLOCKS[0])
    pack_rows(BLOCKS[-1])

    def first_layer(x):
        for r in BLOCKS:
            rows = slice(r, r + 8)
            out = first(fld[0, x, rows], fld[1, x, rows], fld[2, x, rows], fld[3, x, rows], msk[x, rows] == 1)
            for q in range(19):
                main_a[q, x, rows] = out[q]

    def first_four(start):
        def body(i, carry):
            first_layer(start + 2 * i)
            first_layer(start + 2 * i + 1)
            return carry

        lax.fori_loop(0, 2, body, 0)

    def first_side():
        def body(i, carry):
            for r in BLOCKS:
                rows = pl.ds(i * ROWS + r, 8)
                out = first(gfld[0, rows], gfld[1, rows], gfld[2, rows], gfld[3, rows], gmsk[rows] > 0.5)
                for q in range(19):
                    side_a[q, rows] = out[q]
            return carry

        lax.fori_loop(0, 2, body, 0)

    def build_side(start, count, slots, fresh):
        for f in range(5):
            shift_back = 32 * f if f < 4 else 0
            for r in BLOCKS:
                rows = slice(r, r + 8)
                low, high = slice(r, r + 8), slice(ROWS + r, ROWS + r + 8)
                mine = theirs = None
                for i in range(count):
                    x = start + i
                    part = fld[f, x, rows] if f < 4 else msk[x, rows].astype(jnp.float32)
                    part = pltpu.roll(part, lax.rem(8 * x + 4, LANES), 1)
                    mine = part if mine is None else jnp.where(group == x, part, mine)
                for s in slots:
                    part = peer[s, f // 4, rows]
                    part = pltpu.roll(part, lax.rem(32 * s + LANES - shift_back, LANES), 1)
                    theirs = part if theirs is None else jnp.where(lane // 32 == s, part, theirs)
                below = jnp.where(low_half, theirs, mine)
                above = jnp.where(low_half, mine, theirs)
                if not fresh:
                    here = lane // 32 == slots[0]
                    old = (gfld[f, low], gfld[f, high]) if f < 4 else (gmsk[low], gmsk[high])
                    below, above = jnp.where(here, below, old[0]), jnp.where(here, above, old[1])
                if f < 4:
                    gfld[f, low] = below
                    gfld[f, high] = above
                else:
                    gmsk[low] = below
                    gmsk[high] = above

    def pull_main(main, side, x, r):
        f = []
        for q, (cx, cy, cz) in enumerate(VELOCITIES):
            value = main[q, x - cx, r - cy : r - cy + 8]
            if cz == 1:
                edge = pltpu.roll(side[q, r - cy : r - cy + 8], 125 - 8 * (x - cx), 1)
                value = jnp.where(lane == 0, edge, pltpu.roll(value, 1, 1))
            elif cz == -1:
                edge = pltpu.roll(side[q, ROWS + r - cy : ROWS + r - cy + 8], 123 - 8 * (x - cx), 1)
                value = jnp.where(lane == LANES - 1, edge, pltpu.roll(value, LANES - 1, 1))
            f.append(value)
        return f

    def pull_side(side, base, r):
        f = []
        for q, (cx, cy, cz) in enumerate(VELOCITIES):
            value = side[q, pl.ds(base + r - cy, 8)]
            shift = (8 * cx + cz) % LANES
            f.append(pltpu.roll(value, shift, 1) if shift else value)
        return f

    buffers = [(main_a, side_a), (main_b, side_b)]

    def step_layers(step, start, count):
        (main, side), (main_to, _) = buffers[step % 2], buffers[(step + 1) % 2]

        unroll = 4 if count == 4 else 2

        def body(i, carry):
            for k in range(unroll):
                x = start + unroll * i + k
                for r in BLOCKS:
                    rows = slice(r, r + 8)
                    out = collide(pull_main(main, side, x, r), msk[x, rows] == 1)
                    for q in range(19):
                        main_to[q, x, rows] = out[q]
            return carry

        lax.fori_loop(0, count // unroll, body, 0)

    def step_side(step):
        (_, side), (_, side_to) = buffers[step % 2], buffers[(step + 1) % 2]

        def body(i, carry):
            for r in BLOCKS:
                rows = pl.ds(i * ROWS + r, 8)
                out = collide(pull_side(side, i * ROWS, r), gmsk[rows] > 0.5)
                for q in range(19):
                    side_to[q, rows] = out[q]
            return carry

        lax.fori_loop(0, 2, body, 0)

    z_copy = remote(pack.at[:, 4:44], peer.at[1, :, 4:44], z_send, z_recv, z_peer)
    z_copy.start()
    for c in x_copies[3:9]:
        c.start()
    first_four(4)
    for i in range(3):
        x_copies[i].wait_recv()
        f_copies[i].start()
    for c in e_copies[:2]:
        c.start()
    z_copy.wait_recv()
    x_copies[9].start()
    x_copies[3].wait_recv()
    f_copies[3].start()
    for i in range(4, 10):
        x_copies[i].wait_recv()
        f_copies[i].start()
    for c in f_copies[:3]:
        c.wait_recv()
    for c in e_copies[2:]:
        c.start()
    for c in e_copies[:2]:
        c.wait_recv()

    build_side(4 - 4 * par, 8, (1 - par, 2 - par), True)
    first_four(8 - 8 * par)
    first_side()
    step_layers(2, 5 - 4 * par, 6)
    step_side(2)
    step_layers(3, 6 - 4 * par, 4)
    step_side(3)
    step_layers(4, 7 - 4 * par, 2)

    for c in f_copies[3:] + e_copies[2:]:
        c.wait_recv()
    build_side(8 * par, 4, (2 * par,), False)
    first_four(8 * par)
    first_side()
    step_layers(2, 1 + 6 * par, 4)
    step_side(2)
    step_layers(3, 2 + 4 * par, 4)
    step_side(3)
    step_layers(4, 3 + 2 * par, 4)
    step_side(4)

    def last(x):
        for r in INNER:
            rho, m, _, _ = moments(pull_main(main_b, side_b, x, r))
            rows = slice(r - 8, r)
            for k, value in enumerate((rho, *m)):
                out[k, x - 4, rows] = value

    for x in range(4, 8):
        last(x)

    for c in y_copies + [z_copy] + x_copies + f_copies + e_copies:
        c.wait_send()


def split(both, density, momentum, sem):
    copies = [
        pltpu.make_async_copy(both.at[0], density, sem.at[0]),
        pltpu.make_async_copy(both.at[1:4], momentum, sem.at[1]),
    ]
    for c in copies:
        c.start()
    for c in copies:
        c.wait()


def local(density, velocity, solid_mask):
    shape = density.shape
    f32 = jnp.float32
    dma = pltpu.SemaphoreType.DMA
    both = pl.pallas_call(
            kernel,
            out_shape=jax.ShapeDtypeStruct((4,) + shape, f32),
            in_specs=[pl.BlockSpec(memory_space=pl.ANY)] * 3,
            out_specs=pl.BlockSpec(memory_space=pltpu.VMEM),
            scratch_shapes=[
                pltpu.VMEM((4, LAYERS, ROWS, LANES), f32),
                pltpu.VMEM((LAYERS, ROWS, LANES), jnp.int32),
                pltpu.VMEM((2, ROWS, LANES), f32),
                pltpu.VMEM((3, 2, ROWS, LANES), f32),
                pltpu.VMEM((4, 2 * ROWS, LANES), f32),
                pltpu.VMEM((2 * ROWS, LANES), f32),
                pltpu.VMEM((19, LAYERS, ROWS, LANES), f32),
                pltpu.VMEM((19, LAYERS, ROWS, LANES), f32),
                pltpu.VMEM((19, 2 * ROWS, LANES), f32),
                pltpu.VMEM((19, 2 * ROWS, LANES), f32),
                dma((3,)),
                dma((4,)),
                dma((4,)),
                dma,
                dma,
                dma((10,)),
                dma((10,)),
                dma((10,)),
                dma((10,)),
                dma((4,)),
                dma((4,)),
            ],
            compiler_params=pltpu.CompilerParams(collective_id=0, has_side_effects=True, vmem_limit_bytes=51043328),
        )(*[pltpu.with_memory_space_constraint(v, pltpu.HBM) for v in (density, velocity, solid_mask)])
    return tuple(
        pl.pallas_call(
            split,
            out_shape=(jax.ShapeDtypeStruct(shape, f32), jax.ShapeDtypeStruct((3,) + shape, f32)),
            in_specs=[pl.BlockSpec(memory_space=pltpu.VMEM)],
            out_specs=(pl.BlockSpec(memory_space=pl.ANY), pl.BlockSpec(memory_space=pl.ANY)),
            scratch_shapes=[dma((2,))],
            compiler_params=pltpu.CompilerParams(vmem_limit_bytes=32 << 20),
        )(both)
    )


def solution(mesh):
    return jax.shard_map(
        local,
        mesh=mesh,
        in_specs=(P("gx", "gy", "gz"), P(None, "gx", "gy", "gz"), P("gx", "gy", "gz")),
        out_specs=(P("gx", "gy", "gz"), P(None, "gx", "gy", "gz")),
        check_vma=False,
    )
```

```python
import jax
import jax.numpy as jnp
from jax import lax
from jax.experimental import pallas as pl
from jax.experimental.pallas import tpu as pltpu
from jax.sharding import PartitionSpec as P

MESH = pl.DeviceIdType.MESH

VELOCITIES = [
    (0, 0, 0),
    (1, 0, 0),
    (-1, 0, 0),
    (0, 1, 0),
    (0, -1, 0),
    (0, 0, 1),
    (0, 0, -1),
    (1, 1, 0),
    (-1, -1, 0),
    (1, -1, 0),
    (-1, 1, 0),
    (1, 0, 1),
    (-1, 0, -1),
    (1, 0, -1),
    (-1, 0, 1),
    (0, 1, 1),
    (0, -1, -1),
    (0, 1, -1),
    (0, -1, 1),
]
RELAX_RATE = 1.25
W0, W1, W2 = 1.0 / 3.0, 1.0 / 18.0, 1.0 / 36.0

LAYERS, ROWS, LANES = 12, 48, 128
BLOCKS = [4 + 8 * j for j in range(5)]
SIDE = 4


def moments(f):
    s = [f[2 * k + 1] + f[2 * k + 2] for k in range(9)]
    d = [f[2 * k + 1] - f[2 * k + 2] for k in range(9)]
    rho = f[0] + (((s[0] + s[1]) + (s[2] + s[3])) + ((s[4] + s[5]) + (s[6] + s[7]))) + s[8]
    mx = d[0] + (d[3] + d[4]) + (d[5] + d[6])
    my = d[1] + (d[3] - d[4]) + (d[7] + d[8])
    mz = d[2] + (d[5] - d[6]) + (d[7] - d[8])
    return rho, (mx, my, mz), s, d


def balance(rho, m, u, scale):
    mx, my, mz = m
    ux, uy, uz = u
    xx, yy, zz = mx * ux, my * uy, mz * uz
    base = (scale * W2) * rho - (1.0 / 3.0) * (xx + yy + zz)
    px, py, pz = (scale * W2 * 3.0) * mx, (scale * W2 * 3.0) * my, (scale * W2 * 3.0) * mz
    ax, ay, az = base + xx, base + yy, base + zz
    pairs = [(ax + ax, px + px), (ay + ay, py + py), (az + az, pz + pz)]
    mx2, my2 = mx + mx, my + my
    for even, cross, pa, pb in (
        (ax + yy, mx2 * uy, px, py),
        (ax + zz, mx2 * uz, px, pz),
        (ay + zz, my2 * uz, py, pz),
    ):
        pairs.append((even + cross, pa + pb))
        pairs.append((even - cross, pa - pb))
    return (W0 / W2) * base, pairs


def first(rho, vx, vy, vz, solid):
    sign = jnp.where(solid, -1.0, 1.0)
    m = tuple((rho * sign) * v for v in (vx, vy, vz))
    half = jnp.where(solid, -W2 * 4.5, W2 * 4.5)
    rest, pairs = balance(rho, m, tuple(half * v for v in (vx, vy, vz)), 1.0)
    out = [rest]
    for even, odd in pairs:
        out += [even + odd, even - odd]
    return out


def collide(f, solid):
    rho, m, s, d = moments(f)
    inv = (RELAX_RATE * W2 * 4.5) / rho
    u = tuple(v * inv for v in m)
    rho, *m = (jnp.where(solid, 0.0, v) for v in (rho, *m))
    rest, pairs = balance(rho, m, u, RELAX_RATE)
    keep = 1.0 - RELAX_RATE
    keep_rest = jnp.where(solid, 1.0, keep)
    keep_sum = jnp.where(solid, 0.5, 0.5 * keep)
    keep_diff = jnp.where(solid, -0.5, 0.5 * keep)
    out = [keep_rest * f[0] + rest]
    for k, (even, odd) in enumerate(pairs):
        even = even + keep_sum * s[k]
        odd = odd + keep_diff * d[k]
        out += [even + odd, even - odd]
    return out


def kernel(
    density,
    velocity,
    mask,
    out,
    fld,
    msk,
    pack,
    peer,
    gmsk,
    main_a,
    main_b,
    side_a,
    side_b,
    load_sem,
    y_send,
    y_recv,
    z_send,
    z_recv,
    x_send,
    x_recv,
    f_send,
    f_recv,
    e_send,
    e_recv,
):
    gx, gy, gz = lax.axis_index("gx"), lax.axis_index("gy"), lax.axis_index("gz")
    par = lax.rem(gx, 2)
    y_up = (gx, lax.rem(gy + 1, 8), gz)
    y_down = (gx, lax.rem(gy + 7, 8), gz)
    z_peer = (gx, gy, 1 - gz)
    x_peer = (gx + 1 - 2 * par, gy, gz)
    fwd_to = (lax.rem(gx + 2 + 4 * par, 8), gy, gz)
    fwd_from = (lax.rem(gx + 6 - 4 * par, 8), gy, gz)

    loads = [
        pltpu.make_async_copy(density, fld.at[0, 4:8, 8:40], load_sem.at[0]),
        pltpu.make_async_copy(velocity, fld.at[1:4, 4:8, 8:40], load_sem.at[1]),
        pltpu.make_async_copy(mask, msk.at[4:8, 8:40], load_sem.at[2]),
    ]
    for c in loads:
        c.start()

    barrier = pltpu.get_barrier_semaphore()
    for dev in (y_up, y_down, z_peer, x_peer, fwd_to, fwd_from):
        pl.semaphore_signal(barrier, inc=1, device_id=dev, device_id_type=MESH)

    lane = lax.broadcasted_iota(jnp.int32, (8, LANES), 1)
    group = lane // 8
    low_half = lax.rem(lane, 8) < 4

    def field_rows(f, x, r):
        return fld[f, x, r : r + 8] if f < 4 else msk[x, r : r + 8].astype(jnp.float32)

    def columns(f, x):
        acc = None
        for b, r in enumerate(BLOCKS):
            part = pltpu.roll(field_rows(f, x, r), 8 * b + 4, 1)
            acc = part if acc is None else jnp.where(group == b, part, acc)
        return acc

    for c in loads:
        c.wait()
    pl.semaphore_wait(barrier, 6)

    def remote(src, dst, send, recv, dev):
        return pltpu.make_async_remote_copy(
            src_ref=src, dst_ref=dst, send_sem=send, recv_sem=recv, device_id=dev, device_id_type=MESH
        )

    y_copies = [
        remote(fld.at[:, 4:8, 36:40], fld.at[:, 4:8, 4:8], y_send.at[0], y_recv.at[0], y_up),
        remote(fld.at[:, 4:8, 8:12], fld.at[:, 4:8, 40:44], y_send.at[1], y_recv.at[1], y_down),
        remote(msk.at[4:8, 36:40], msk.at[4:8, 4:8], y_send.at[2], y_recv.at[2], y_up),
        remote(msk.at[4:8, 8:12], msk.at[4:8, 40:44], y_send.at[3], y_recv.at[3], y_down),
    ]
    for c in y_copies:
        c.start()

    near = 8 * (1 - par)
    far = 8 * par
    near_slot, far_slot = 2 * (1 - par), 2 * par

    def parts(start, slot):
        layers = pl.ds(start, 4)
        refs = [fld.at[f, layers, 8:40] for f in range(3)]
        refs += [fld.at[3, layers, 4:44], msk.at[pl.ds(start, 2), 4:44], msk.at[pl.ds(start + 2, 2), 4:44]]
        refs += [peer.at[slot]]
        return refs

    x_copies = [
        remote(a, b, x_send.at[i], x_recv.at[i], x_peer)
        for i, (a, b) in enumerate(zip(parts(4, 1), parts(far, far_slot)))
    ]
    f_copies = [
        remote(a, b, f_send.at[i], f_recv.at[i], fwd_to)
        for i, (a, b) in enumerate(zip(parts(near, near_slot), parts(far, far_slot)))
    ]
    e_copies = []
    for i, layers in enumerate((pl.ds(near, 4), pl.ds(far, 4))):
        up, down = fld.at[0:3, layers, 36:40], fld.at[0:3, layers, 8:12]
        e_copies += [
            remote(up, fld.at[0:3, layers, 4:8], e_send.at[2 * i], e_recv.at[2 * i], y_up),
            remote(down, fld.at[0:3, layers, 40:44], e_send.at[2 * i + 1], e_recv.at[2 * i + 1], y_down),
        ]
    for c in x_copies[:3]:
        c.start()
    for c in y_copies:
        c.wait_recv()
    for v in range(7):
        acc = None
        for k, m in enumerate(range(3 * v, min(3 * v + 3, 20))):
            part = columns(m // 4, 4 + m % 4)
            part = pltpu.roll(part, 40 * k, 1) if k else part
            acc = part if acc is None else jnp.where(group >= 5 * k, part, acc)
        pack[v] = acc

    def first_four(start):
        def body(i, carry):
            for x in (start + 2 * i, start + 2 * i + 1):
                for r in BLOCKS:
                    rows = slice(r, r + 8)
                    out = first(fld[0, x, rows], fld[1, x, rows], fld[2, x, rows], fld[3, x, rows], msk[x, rows] == 1)
                    for q in range(19):
                        main_a[q, x, rows] = out[q]
            return carry

        lax.fori_loop(0, 2, body, 0)

    def store_side(side, x, out):
        for q, (_, cy, _) in enumerate(VELOCITIES):
            side[q, x, SIDE : SIDE + 8] = out[q]
            if cy == 1:
                side[q, x, SIDE - 1 : SIDE] = pltpu.roll(out[q], 8, 1)[7:8]
            elif cy == -1:
                side[q, x, SIDE + 8 : SIDE + 9] = pltpu.roll(out[q], LANES - 8, 1)[0:1]

    def first_side(start, slot):
        for i in range(4):
            x = start + i
            cells = []
            for f in range(5):
                m = 4 * f + i
                mine = columns(f, x)
                theirs = peer[slot, m // 3]
                theirs = pltpu.roll(theirs, LANES - 40 * (m % 3), 1) if m % 3 else theirs
                above = pltpu.roll(jnp.where(low_half, mine, theirs), 64, 1)
                cells.append(jnp.where(lane < 64, jnp.where(low_half, theirs, mine), above))
            gmsk[x] = cells[4]
            store_side(side_a, x, first(*cells[:4], cells[4] > 0.5))

    def pull_main(main, side, x, b):
        f = []
        r = BLOCKS[b]
        for q, (cx, cy, cz) in enumerate(VELOCITIES):
            value = main[q, x - cx, r - cy : r - cy + 8]
            if cz:
                edge = side[q, x - cx, SIDE - cy : SIDE - cy + 8]
                if cz == 1:
                    edge = pltpu.roll(edge, (125 - 8 * b) % LANES, 1)
                    value = jnp.where(lane == 0, edge, pltpu.roll(value, 1, 1))
                else:
                    edge = pltpu.roll(edge, 59 - 8 * b, 1)
                    value = jnp.where(lane == LANES - 1, edge, pltpu.roll(value, LANES - 1, 1))
            f.append(value)
        return f

    def pull_side(side, x):
        f = []
        for q, (cx, cy, cz) in enumerate(VELOCITIES):
            value = side[q, x - cx, SIDE - cy : SIDE - cy + 8]
            f.append(pltpu.roll(value, cz % LANES, 1) if cz else value)
        return f

    buffers = [(main_a, side_a), (main_b, side_b)]

    def step_layers(step, start, count):
        (main, side), (main_to, side_to) = buffers[step % 2], buffers[(step + 1) % 2]
        unroll = 2

        def body(i, carry):
            for k in range(unroll):
                x = start + unroll * i + k
                store_side(side_to, x, collide(pull_side(side, x), gmsk[x] > 0.5))
            for k in range(unroll):
                x = start + unroll * i + k
                for b, r in enumerate(BLOCKS):
                    rows = slice(r, r + 8)
                    out = collide(pull_main(main, side, x, b), msk[x, rows] == 1)
                    for q in range(19):
                        main_to[q, x, rows] = out[q]
            return carry

        lax.fori_loop(0, count // unroll, body, 0)

    z_copy = remote(pack, peer.at[1], z_send, z_recv, z_peer)
    z_copy.start()
    for c in x_copies[3:6]:
        c.start()
    first_four(4)
    for i in range(3):
        x_copies[i].wait_recv()
        f_copies[i].start()
    for c in e_copies[:2]:
        c.start()
    z_copy.wait_recv()
    x_copies[6].start()
    x_copies[3].wait_recv()
    f_copies[3].start()
    for i in range(4, 7):
        x_copies[i].wait_recv()
        f_copies[i].start()
    for c in f_copies[:3]:
        c.wait_recv()
    for c in e_copies[2:]:
        c.start()
    for c in e_copies[:2]:
        c.wait_recv()

    first_side(4, 1)
    first_four(8 - 8 * par)
    first_side(8 - 8 * par, near_slot)
    step_layers(2, 5 - 4 * par, 6)
    step_layers(3, 6 - 4 * par, 4)
    step_layers(4, 7 - 4 * par, 2)

    for c in f_copies[3:] + e_copies[2:]:
        c.wait_recv()
    first_four(8 * par)
    first_side(8 * par, far_slot)
    step_layers(2, 1 + 6 * par, 4)
    step_layers(3, 2 + 4 * par, 4)
    step_layers(4, 3 + 2 * par, 4)

    def pull(ref, x, row, cz):
        part = {c[:2]: ref[q, x - c[0], row - c[1] : row - c[1] + 8] for q, c in enumerate(VELOCITIES) if c[2] == cz}
        sums = [part[0, 0], part[1, 0] - part[-1, 0], part[0, 1] - part[0, -1]]
        sums[0] += (part[1, 0] + part[-1, 0]) + (part[0, 1] + part[0, -1])
        if not cz:
            diagonal = [part[1, 1], part[-1, -1], part[1, -1], part[-1, 1]]
            sums[0] += (diagonal[0] + diagonal[1]) + (diagonal[2] + diagonal[3])
            sums[1] += (diagonal[0] - diagonal[1]) + (diagonal[2] - diagonal[3])
            sums[2] += (diagonal[0] - diagonal[1]) - (diagonal[2] - diagonal[3])
        return sums

    def moved(x, b, cz):
        row = BLOCKS[b]
        shift, edge_lane = ((125 - 8 * b) % LANES, 0) if cz == 1 else (59 - 8 * b, LANES - 1)
        result = []
        for value, edge in zip(pull(main_b, x, row, cz), pull(side_b, x, SIDE, cz)):
            value = pltpu.roll(value, cz % LANES, 1)
            result.append(jnp.where(lane == edge_lane, pltpu.roll(edge, shift, 1), value))
        return result

    def last(i, carry):
        for x in [4 + 4 * i + k for k in range(4)]:
            for b, r in enumerate(BLOCKS):
                rest, up, down = pull(main_b, x, r, 0), moved(x, b, 1), moved(x, b, -1)
                rho, mx, my = (rest[k] + (up[k] + down[k]) for k in range(3))
                low, high = max(r, 8), min(r + 8, 40)
                for k, value in enumerate((rho, mx, my, up[0] - down[0])):
                    out[k, x - 4, low - 8 : high - 8] = value[low - r : high - r]
        return carry

    lax.fori_loop(0, 4 // 4, last, 0)

    for c in y_copies + [z_copy] + x_copies + f_copies + e_copies:
        c.wait_send()


def split(both, density, momentum, sem):
    copies = [
        pltpu.make_async_copy(both.at[0], density, sem.at[0]),
        pltpu.make_async_copy(both.at[1:4], momentum, sem.at[1]),
    ]
    for c in copies:
        c.start()
    for c in copies:
        c.wait()


def local(density, velocity, solid_mask):
    shape = density.shape
    f32 = jnp.float32
    dma = pltpu.SemaphoreType.DMA
    both = pl.pallas_call(
            kernel,
            out_shape=jax.ShapeDtypeStruct((4,) + shape, f32),
            in_specs=[pl.BlockSpec(memory_space=pl.ANY)] * 3,
            out_specs=pl.BlockSpec(memory_space=pltpu.VMEM),
            scratch_shapes=[
                pltpu.VMEM((4, LAYERS, ROWS, LANES), f32),
                pltpu.VMEM((LAYERS, ROWS, LANES), jnp.int32),
                pltpu.VMEM((7, 8, LANES), f32),
                pltpu.VMEM((3, 7, 8, LANES), f32),
                pltpu.VMEM((LAYERS, 8, LANES), f32),
                pltpu.VMEM((19, LAYERS, ROWS, LANES), f32),
                pltpu.VMEM((19, LAYERS, ROWS, LANES), f32),
                pltpu.VMEM((19, LAYERS, 16, LANES), f32),
                pltpu.VMEM((19, LAYERS, 16, LANES), f32),
                dma((3,)),
                dma((4,)),
                dma((4,)),
                dma,
                dma,
                dma((7,)),
                dma((7,)),
                dma((7,)),
                dma((7,)),
                dma((4,)),
                dma((4,)),
            ],
            compiler_params=pltpu.CompilerParams(collective_id=0, has_side_effects=True, vmem_limit_bytes=51043328),
        )(*[pltpu.with_memory_space_constraint(v, pltpu.HBM) for v in (density, velocity, solid_mask)])
    return tuple(
        pl.pallas_call(
            split,
            out_shape=(jax.ShapeDtypeStruct(shape, f32), jax.ShapeDtypeStruct((3,) + shape, f32)),
            in_specs=[pl.BlockSpec(memory_space=pltpu.VMEM)],
            out_specs=(pl.BlockSpec(memory_space=pl.ANY), pl.BlockSpec(memory_space=pl.ANY)),
            scratch_shapes=[dma((2,))],
            compiler_params=pltpu.CompilerParams(vmem_limit_bytes=32 << 20),
        )(both)
    )


def solution(mesh):
    return jax.shard_map(
        local,
        mesh=mesh,
        in_specs=(P("gx", "gy", "gz"), P(None, "gx", "gy", "gz"), P("gx", "gy", "gz")),
        out_specs=(P("gx", "gy", "gz"), P(None, "gx", "gy", "gz")),
        check_vma=False,
    )
```

```python
import jax
import jax.numpy as jnp
from jax import lax
from jax.experimental import pallas as pl
from jax.experimental.pallas import tpu as pltpu
from jax.sharding import PartitionSpec as P

MESH = pl.DeviceIdType.MESH

VELOCITIES = [
    (0, 0, 0),
    (1, 0, 0),
    (-1, 0, 0),
    (0, 1, 0),
    (0, -1, 0),
    (0, 0, 1),
    (0, 0, -1),
    (1, 1, 0),
    (-1, -1, 0),
    (1, -1, 0),
    (-1, 1, 0),
    (1, 0, 1),
    (-1, 0, -1),
    (1, 0, -1),
    (-1, 0, 1),
    (0, 1, 1),
    (0, -1, -1),
    (0, 1, -1),
    (0, -1, 1),
]
RELAX_RATE = 1.25
W0, W1, W2 = 1.0 / 3.0, 1.0 / 18.0, 1.0 / 36.0

LAYERS, ROWS, LANES = 12, 48, 128
BLOCKS = [4 + 8 * j for j in range(5)]
SIDE = 4


def moments(f):
    s = [f[2 * k + 1] + f[2 * k + 2] for k in range(9)]
    d = [f[2 * k + 1] - f[2 * k + 2] for k in range(9)]
    rho = f[0] + (((s[0] + s[1]) + (s[2] + s[3])) + ((s[4] + s[5]) + (s[6] + s[7]))) + s[8]
    mx = d[0] + (d[3] + d[4]) + (d[5] + d[6])
    my = d[1] + (d[3] - d[4]) + (d[7] + d[8])
    mz = d[2] + (d[5] - d[6]) + (d[7] - d[8])
    return rho, (mx, my, mz), s, d


def balance(rho, m, u, scale):
    mx, my, mz = m
    ux, uy, uz = u
    xx, yy, zz = mx * ux, my * uy, mz * uz
    base = (scale * W2) * rho - (1.0 / 3.0) * (xx + yy + zz)
    px, py, pz = (scale * W2 * 3.0) * mx, (scale * W2 * 3.0) * my, (scale * W2 * 3.0) * mz
    ax, ay, az = base + xx, base + yy, base + zz
    pairs = [(ax + ax, px + px), (ay + ay, py + py), (az + az, pz + pz)]
    mx2, my2 = mx + mx, my + my
    for even, cross, pa, pb in (
        (ax + yy, mx2 * uy, px, py),
        (ax + zz, mx2 * uz, px, pz),
        (ay + zz, my2 * uz, py, pz),
    ):
        pairs.append((even + cross, pa + pb))
        pairs.append((even - cross, pa - pb))
    return (W0 / W2) * base, pairs


def first(rho, vx, vy, vz, solid):
    sign = jnp.where(solid, -1.0, 1.0)
    m = tuple((rho * sign) * v for v in (vx, vy, vz))
    half = jnp.where(solid, -W2 * 4.5, W2 * 4.5)
    rest, pairs = balance(rho, m, tuple(half * v for v in (vx, vy, vz)), 1.0)
    out = [rest]
    for even, odd in pairs:
        out += [even + odd, even - odd]
    return out


def collide(f, solid):
    rho, m, s, d = moments(f)
    inv = (RELAX_RATE * W2 * 4.5) / rho
    u = tuple(v * inv for v in m)
    rho, *m = (jnp.where(solid, 0.0, v) for v in (rho, *m))
    rest, pairs = balance(rho, m, u, RELAX_RATE)
    keep = 1.0 - RELAX_RATE
    keep_rest = jnp.where(solid, 1.0, keep)
    keep_sum = jnp.where(solid, 0.5, 0.5 * keep)
    keep_diff = jnp.where(solid, -0.5, 0.5 * keep)
    out = [keep_rest * f[0] + rest]
    for k, (even, odd) in enumerate(pairs):
        even = even + keep_sum * s[k]
        odd = odd + keep_diff * d[k]
        out += [even + odd, even - odd]
    return out


def kernel(
    density,
    velocity,
    mask,
    out,
    fld,
    msk,
    pack,
    peer,
    gmsk,
    main_a,
    main_b,
    side_a,
    side_b,
    load_sem,
    y_send,
    y_recv,
    z_send,
    z_recv,
    x_send,
    x_recv,
    f_send,
    f_recv,
    e_send,
    e_recv,
):
    gx, gy, gz = lax.axis_index("gx"), lax.axis_index("gy"), lax.axis_index("gz")
    par = lax.rem(gx, 2)
    y_up = (gx, lax.rem(gy + 1, 8), gz)
    y_down = (gx, lax.rem(gy + 7, 8), gz)
    z_peer = (gx, gy, 1 - gz)
    x_peer = (gx + 1 - 2 * par, gy, gz)
    fwd_to = (lax.rem(gx + 2 + 4 * par, 8), gy, gz)
    fwd_from = (lax.rem(gx + 6 - 4 * par, 8), gy, gz)

    loads = [
        pltpu.make_async_copy(density, fld.at[0, 4:8, 8:40], load_sem.at[0]),
        pltpu.make_async_copy(velocity, fld.at[1:4, 4:8, 8:40], load_sem.at[1]),
        pltpu.make_async_copy(mask, msk.at[4:8, 8:40], load_sem.at[2]),
    ]
    for c in loads:
        c.start()

    barrier = pltpu.get_barrier_semaphore()
    for dev in (y_up, y_down, z_peer, x_peer, fwd_to, fwd_from):
        pl.semaphore_signal(barrier, inc=1, device_id=dev, device_id_type=MESH)

    lane = lax.broadcasted_iota(jnp.int32, (8, LANES), 1)
    group = lane // 8
    low_half = lax.rem(lane, 8) < 4

    def field_rows(f, x, r):
        return fld[f, x, r : r + 8] if f < 4 else msk[x, r : r + 8].astype(jnp.float32)

    def columns(f, x):
        acc = None
        for b, r in enumerate(BLOCKS):
            part = pltpu.roll(field_rows(f, x, r), 8 * b + 4, 1)
            acc = part if acc is None else jnp.where(group == b, part, acc)
        return acc

    for c in loads:
        c.wait()
    pl.semaphore_wait(barrier, 6)

    def remote(src, dst, send, recv, dev):
        return pltpu.make_async_remote_copy(
            src_ref=src, dst_ref=dst, send_sem=send, recv_sem=recv, device_id=dev, device_id_type=MESH
        )

    y_copies = [
        remote(fld.at[:, 4:8, 36:40], fld.at[:, 4:8, 4:8], y_send.at[0], y_recv.at[0], y_up),
        remote(fld.at[:, 4:8, 8:12], fld.at[:, 4:8, 40:44], y_send.at[1], y_recv.at[1], y_down),
        remote(msk.at[4:8, 36:40], msk.at[4:8, 4:8], y_send.at[2], y_recv.at[2], y_up),
        remote(msk.at[4:8, 8:12], msk.at[4:8, 40:44], y_send.at[3], y_recv.at[3], y_down),
    ]
    for c in y_copies:
        c.start()

    near = 8 * (1 - par)
    far = 8 * par
    near_slot, far_slot = 2 * (1 - par), 2 * par

    def parts(start, slot):
        layers = pl.ds(start, 4)
        refs = [fld.at[f, layers, 8:40] for f in range(3)] + [fld.at[f, layers, 4:44] for f in range(3, 4)]
        refs += [msk.at[pl.ds(start, 2), 4:44], msk.at[pl.ds(start + 2, 2), 4:44]]
        refs += [peer.at[slot]]
        return refs

    x_copies = [
        remote(a, b, x_send.at[i], x_recv.at[i], x_peer)
        for i, (a, b) in enumerate(zip(parts(4, 1), parts(far, far_slot)))
    ]
    f_copies = [
        remote(a, b, f_send.at[i], f_recv.at[i], fwd_to)
        for i, (a, b) in enumerate(zip(parts(near, near_slot), parts(far, far_slot)))
    ]
    e_copies = []
    for i, layers in enumerate((pl.ds(near, 4), pl.ds(far, 4))):
        up, down = fld.at[0:3, layers, 36:40], fld.at[0:3, layers, 8:12]
        e_copies += [
            remote(up, fld.at[0:3, layers, 4:8], e_send.at[2 * i], e_recv.at[2 * i], y_up),
            remote(down, fld.at[0:3, layers, 40:44], e_send.at[2 * i + 1], e_recv.at[2 * i + 1], y_down),
        ]
    for c in x_copies[:3]:
        c.start()
    for c in y_copies:
        c.wait_recv()
    for v in range(7):
        acc = None
        for k, m in enumerate(range(3 * v, min(3 * v + 3, 20))):
            part = columns(m // 4, 4 + m % 4)
            part = pltpu.roll(part, 40 * k, 1) if k else part
            acc = part if acc is None else jnp.where(group >= 5 * k, part, acc)
        pack[v] = acc

    def first_four(start):
        def body(i, carry):
            for x in (start + 2 * i, start + 2 * i + 1):
                for r in BLOCKS:
                    rows = slice(r, r + 8)
                    out = first(fld[0, x, rows], fld[1, x, rows], fld[2, x, rows], fld[3, x, rows], msk[x, rows] == 1)
                    for q in range(19):
                        main_a[q, x, rows] = out[q]
            return carry

        lax.fori_loop(0, 2, body, 0)

    def store_side(side, x, out):
        for q, (_, cy, _) in enumerate(VELOCITIES):
            side[q, x, SIDE : SIDE + 8] = out[q]
            if cy == 1:
                side[q, x, SIDE - 1 : SIDE] = pltpu.roll(out[q], 8, 1)[7:8]
            elif cy == -1:
                side[q, x, SIDE + 8 : SIDE + 9] = pltpu.roll(out[q], LANES - 8, 1)[0:1]

    def first_side(start, slot):
        for i in range(4):
            x = start + i
            cells = []
            for f in range(5):
                m = 4 * f + i
                mine = columns(f, x)
                theirs = peer[slot, m // 3]
                theirs = pltpu.roll(theirs, LANES - 40 * (m % 3), 1) if m % 3 else theirs
                above = pltpu.roll(jnp.where(low_half, mine, theirs), 64, 1)
                cells.append(jnp.where(lane < 64, jnp.where(low_half, theirs, mine), above))
            gmsk[x] = cells[4]
            store_side(side_a, x, first(*cells[:4], cells[4] > 0.5))

    def pull_main(main, side, x, b):
        f = []
        r = BLOCKS[b]
        for q, (cx, cy, cz) in enumerate(VELOCITIES):
            value = main[q, x - cx, r - cy : r - cy + 8]
            if cz:
                edge = side[q, x - cx, SIDE - cy : SIDE - cy + 8]
                if cz == 1:
                    edge = pltpu.roll(edge, (125 - 8 * b) % LANES, 1)
                    value = jnp.where(lane == 0, edge, pltpu.roll(value, 1, 1))
                else:
                    edge = pltpu.roll(edge, 59 - 8 * b, 1)
                    value = jnp.where(lane == LANES - 1, edge, pltpu.roll(value, LANES - 1, 1))
            f.append(value)
        return f

    def pull_side(side, x):
        f = []
        for q, (cx, cy, cz) in enumerate(VELOCITIES):
            value = side[q, x - cx, SIDE - cy : SIDE - cy + 8]
            f.append(pltpu.roll(value, cz % LANES, 1) if cz else value)
        return f

    buffers = [(main_a, side_a), (main_b, side_b)]

    def step_layers(step, start, count):
        (main, side), (main_to, side_to) = buffers[step % 2], buffers[(step + 1) % 2]
        unroll = 2

        def body(i, carry):
            x = start + 2 * i + 0
            store_side(side_to, x, collide(pull_side(side, x), gmsk[x] > 0.5))
            x = start + 2 * i + 0
            for b, r in [(b, BLOCKS[b]) for b in [0, 1, 2, 3, 4]]:
                rows = slice(r, r + 8)
                out = collide(pull_main(main, side, x, b), msk[x, rows] == 1)
                for q in range(19):
                    main_to[q, x, rows] = out[q]
            x = start + 2 * i + 1
            for b, r in [(b, BLOCKS[b]) for b in [0, 1, 2, 3, 4]]:
                rows = slice(r, r + 8)
                out = collide(pull_main(main, side, x, b), msk[x, rows] == 1)
                for q in range(19):
                    main_to[q, x, rows] = out[q]
            x = start + 2 * i + 1
            store_side(side_to, x, collide(pull_side(side, x), gmsk[x] > 0.5))
            return carry

        lax.fori_loop(0, count // unroll, body, 0)

    z_copy = remote(pack, peer.at[1], z_send, z_recv, z_peer)
    z_copy.start()
    for c in x_copies[3:6]:
        c.start()
    first_four(4)
    x_copies[0].wait_recv()
    f_copies[0].start()
    x_copies[1].wait_recv()
    f_copies[1].start()
    x_copies[2].wait_recv()
    f_copies[2].start()
    for c in e_copies[:2]:
        c.start()
    z_copy.wait_recv()
    x_copies[6].start()
    x_copies[3].wait_recv()
    f_copies[3].start()
    x_copies[4].wait_recv()
    f_copies[4].start()
    for c in f_copies[:3]:
        c.wait_recv()
    for c in e_copies[2:]:
        c.start()
    x_copies[5].wait_recv()
    f_copies[5].start()
    x_copies[6].wait_recv()
    f_copies[6].start()
    for c in e_copies[:2]:
        c.wait_recv()

    first_side(4, 1)
    first_four(8 - 8 * par)
    first_side(8 - 8 * par, near_slot)
    step_layers(2, 5 - 4 * par, 6)
    step_layers(3, 6 - 4 * par, 4)
    step_layers(4, 7 - 4 * par, 2)

    for c in f_copies[3:6] + e_copies[2:]:
        c.wait_recv()
    first_four(8 * par)
    f_copies[6].wait_recv()
    first_side(8 * par, far_slot)
    step_layers(2, 1 + 6 * par, 4)
    step_layers(3, 2 + 4 * par, 4)
    step_layers(4, 3 + 2 * par, 4)

    def pull(ref, x, row, cz):
        part = {c[:2]: ref[q, x - c[0], row - c[1] : row - c[1] + 8] for q, c in enumerate(VELOCITIES) if c[2] == cz}
        sums = [part[0, 0], part[1, 0] - part[-1, 0], part[0, 1] - part[0, -1]]
        sums[0] += (part[1, 0] + part[-1, 0]) + (part[0, 1] + part[0, -1])
        if not cz:
            diagonal = [part[1, 1], part[-1, -1], part[1, -1], part[-1, 1]]
            sums[0] += (diagonal[0] + diagonal[1]) + (diagonal[2] + diagonal[3])
            sums[1] += (diagonal[0] - diagonal[1]) + (diagonal[2] - diagonal[3])
            sums[2] += (diagonal[0] - diagonal[1]) - (diagonal[2] - diagonal[3])
        return sums

    def moved(x, b, cz):
        row = BLOCKS[b]
        shift, edge_lane = ((125 - 8 * b) % LANES, 0) if cz == 1 else (59 - 8 * b, LANES - 1)
        result = []
        for value, edge in zip(pull(main_b, x, row, cz), pull(side_b, x, SIDE, cz)):
            value = pltpu.roll(value, cz % LANES, 1)
            result.append(jnp.where(lane == edge_lane, pltpu.roll(edge, shift, 1), value))
        return result

    def last(i, carry):
        for x in [4 + 4 * i + k for k in range(4)]:
            for b, r in enumerate(BLOCKS):
                rest, up, down = pull(main_b, x, r, 0), moved(x, b, 1), moved(x, b, -1)
                rho, mx, my = (rest[k] + (up[k] + down[k]) for k in range(3))
                low, high = max(r, 8), min(r + 8, 40)
                for k, value in enumerate((rho, mx, my, up[0] - down[0])):
                    out[k, x - 4, low - 8 : high - 8] = value[low - r : high - r]
        return carry

    lax.fori_loop(0, 4 // 4, last, 0)

    for c in y_copies + [z_copy] + x_copies + f_copies + e_copies:
        c.wait_send()


def split(both, density, momentum, sem):
    copies = [
        pltpu.make_async_copy(both.at[0], density, sem.at[0]),
        pltpu.make_async_copy(both.at[1:4], momentum, sem.at[1]),
    ]
    for c in copies:
        c.start()
    for c in copies:
        c.wait()


def local(density, velocity, solid_mask):
    shape = density.shape
    f32 = jnp.float32
    dma = pltpu.SemaphoreType.DMA
    both = pl.pallas_call(
            kernel,
            out_shape=jax.ShapeDtypeStruct((4,) + shape, f32),
            in_specs=[pl.BlockSpec(memory_space=pl.ANY)] * 3,
            out_specs=pl.BlockSpec(memory_space=pltpu.VMEM),
            scratch_shapes=[
                pltpu.VMEM((4, LAYERS, ROWS, LANES), f32),
                pltpu.VMEM((LAYERS, ROWS, LANES), jnp.int32),
                pltpu.VMEM((7, 8, LANES), f32),
                pltpu.VMEM((3, 7, 8, LANES), f32),
                pltpu.VMEM((LAYERS, 8, LANES), f32),
                pltpu.VMEM((19, LAYERS, ROWS, LANES), f32),
                pltpu.VMEM((19, LAYERS, ROWS, LANES), f32),
                pltpu.VMEM((19, LAYERS, 16, LANES), f32),
                pltpu.VMEM((19, LAYERS, 16, LANES), f32),
                dma((3,)),
                dma((4,)),
                dma((4,)),
                dma,
                dma,
                dma((7,)),
                dma((7,)),
                dma((7,)),
                dma((7,)),
                dma((4,)),
                dma((4,)),
            ],
            compiler_params=pltpu.CompilerParams(collective_id=0, has_side_effects=True, vmem_limit_bytes=51043328),
        )(*[pltpu.with_memory_space_constraint(v, pltpu.HBM) for v in (density, velocity, solid_mask)])
    return tuple(
        pl.pallas_call(
            split,
            out_shape=(jax.ShapeDtypeStruct(shape, f32), jax.ShapeDtypeStruct((3,) + shape, f32)),
            in_specs=[pl.BlockSpec(memory_space=pltpu.VMEM)],
            out_specs=(pl.BlockSpec(memory_space=pl.ANY), pl.BlockSpec(memory_space=pl.ANY)),
            scratch_shapes=[dma((2,))],
            compiler_params=pltpu.CompilerParams(vmem_limit_bytes=32 << 20),
        )(both)
    )


def solution(mesh):
    return jax.shard_map(
        local,
        mesh=mesh,
        in_specs=(P("gx", "gy", "gz"), P(None, "gx", "gy", "gz"), P("gx", "gy", "gz")),
        out_specs=(P("gx", "gy", "gz"), P(None, "gx", "gy", "gz")),
        check_vma=False,
    )
```

```python
import jax
import jax.numpy as jnp
from jax import lax
from jax.experimental import pallas as pl
from jax.experimental.pallas import tpu as pltpu
from jax.sharding import PartitionSpec as P

MESH = pl.DeviceIdType.MESH

VELOCITIES = [
    (0, 0, 0),
    (1, 0, 0),
    (-1, 0, 0),
    (0, 1, 0),
    (0, -1, 0),
    (0, 0, 1),
    (0, 0, -1),
    (1, 1, 0),
    (-1, -1, 0),
    (1, -1, 0),
    (-1, 1, 0),
    (1, 0, 1),
    (-1, 0, -1),
    (1, 0, -1),
    (-1, 0, 1),
    (0, 1, 1),
    (0, -1, -1),
    (0, 1, -1),
    (0, -1, 1),
]
RELAX_RATE = 1.25
W0, W1, W2 = 1.0 / 3.0, 1.0 / 18.0, 1.0 / 36.0

LAYERS, ROWS, LANES = 12, 48, 128
BLOCKS = [4 + 8 * j for j in range(5)]
SIDE = 8


def moments(f):
    s = [f[2 * k + 1] + f[2 * k + 2] for k in range(9)]
    d = [f[2 * k + 1] - f[2 * k + 2] for k in range(9)]
    rho = f[0] + (((s[0] + s[1]) + (s[2] + s[3])) + ((s[4] + s[5]) + (s[6] + s[7]))) + s[8]
    mx = d[0] + (d[3] + d[4]) + (d[5] + d[6])
    my = d[1] + (d[3] - d[4]) + (d[7] + d[8])
    mz = d[2] + (d[5] - d[6]) + (d[7] - d[8])
    return rho, (mx, my, mz), s, d


def balance(rho, m, u, scale):
    mx, my, mz = m
    ux, uy, uz = u
    xx, yy, zz = mx * ux, my * uy, mz * uz
    base = (scale * W2) * rho - (1.0 / 3.0) * (xx + yy + zz)
    px, py, pz = (scale * W2 * 3.0) * mx, (scale * W2 * 3.0) * my, (scale * W2 * 3.0) * mz
    ax, ay, az = base + xx, base + yy, base + zz
    pairs = [(ax + ax, px + px), (ay + ay, py + py), (az + az, pz + pz)]
    mx2, my2 = mx + mx, my + my
    for even, cross, pa, pb in (
        (ax + yy, mx2 * uy, px, py),
        (ax + zz, mx2 * uz, px, pz),
        (ay + zz, my2 * uz, py, pz),
    ):
        pairs.append((even + cross, pa + pb))
        pairs.append((even - cross, pa - pb))
    return (W0 / W2) * base, pairs


def first(rho, vx, vy, vz, solid):
    sign = jnp.where(solid, -1.0, 1.0)
    m = tuple((rho * sign) * v for v in (vx, vy, vz))
    half = jnp.where(solid, -W2 * 4.5, W2 * 4.5)
    rest, pairs = balance(rho, m, tuple(half * v for v in (vx, vy, vz)), 1.0)
    out = [rest]
    for even, odd in pairs:
        out += [even + odd, even - odd]
    return out


def collide(f, solid):
    rho, m, s, d = moments(f)
    inv = (RELAX_RATE * W2 * 4.5) / rho
    u = tuple(v * inv for v in m)
    rho, *m = (jnp.where(solid, 0.0, v) for v in (rho, *m))
    rest, pairs = balance(rho, m, u, RELAX_RATE)
    keep = 1.0 - RELAX_RATE
    keep_rest = jnp.where(solid, 1.0, keep)
    keep_sum = jnp.where(solid, 0.5, 0.5 * keep)
    keep_diff = jnp.where(solid, -0.5, 0.5 * keep)
    out = [keep_rest * f[0] + rest]
    for k, (even, odd) in enumerate(pairs):
        even = even + keep_sum * s[k]
        odd = odd + keep_diff * d[k]
        out += [even + odd, even - odd]
    return out


def kernel(
    density,
    velocity,
    mask,
    out,
    fld,
    msk,
    pack,
    peer,
    gmsk,
    main_a,
    main_b,
    side_a,
    side_b,
    load_sem,
    y_send,
    y_recv,
    z_send,
    z_recv,
    x_send,
    x_recv,
    f_send,
    f_recv,
    e_send,
    e_recv,
):
    gx, gy, gz = lax.axis_index("gx"), lax.axis_index("gy"), lax.axis_index("gz")
    par = lax.rem(gx, 2)
    y_up = (gx, lax.rem(gy + 1, 8), gz)
    y_down = (gx, lax.rem(gy + 7, 8), gz)
    z_peer = (gx, gy, 1 - gz)
    x_peer = (gx + 1 - 2 * par, gy, gz)
    fwd_to = (lax.rem(gx + 2 + 4 * par, 8), gy, gz)
    fwd_from = (lax.rem(gx + 6 - 4 * par, 8), gy, gz)

    loads = [
        pltpu.make_async_copy(density, fld.at[0, 4:8, 8:40], load_sem.at[0]),
        pltpu.make_async_copy(velocity, fld.at[1:4, 4:8, 8:40], load_sem.at[1]),
        pltpu.make_async_copy(mask, msk.at[4:8, 8:40], load_sem.at[2]),
    ]
    for c in loads:
        c.start()

    barrier = pltpu.get_barrier_semaphore()
    for dev in (y_up, y_down, z_peer, x_peer, fwd_to, fwd_from):
        pl.semaphore_signal(barrier, inc=1, device_id=dev, device_id_type=MESH)

    lane = lax.broadcasted_iota(jnp.int32, (8, LANES), 1)
    group = lane // 8
    low_half = lax.rem(lane, 8) < 4

    def field_rows(f, x, r):
        return fld[f, x, r : r + 8] if f < 4 else msk[x, r : r + 8].astype(jnp.float32)

    def columns(f, x):
        acc = None
        for b, r in enumerate(BLOCKS):
            part = pltpu.roll(field_rows(f, x, r), 8 * b + 4, 1)
            acc = part if acc is None else jnp.where(group == b, part, acc)
        return acc

    for c in loads:
        c.wait()
    pl.semaphore_wait(barrier, 6)

    def remote(src, dst, send, recv, dev):
        return pltpu.make_async_remote_copy(
            src_ref=src, dst_ref=dst, send_sem=send, recv_sem=recv, device_id=dev, device_id_type=MESH
        )

    y_copies = [
        remote(fld.at[:, 4:8, 36:40], fld.at[:, 4:8, 4:8], y_send.at[0], y_recv.at[0], y_up),
        remote(fld.at[:, 4:8, 8:12], fld.at[:, 4:8, 40:44], y_send.at[1], y_recv.at[1], y_down),
        remote(msk.at[4:8, 36:40], msk.at[4:8, 4:8], y_send.at[2], y_recv.at[2], y_up),
        remote(msk.at[4:8, 8:12], msk.at[4:8, 40:44], y_send.at[3], y_recv.at[3], y_down),
    ]
    for c in y_copies:
        c.start()

    near = 8 * (1 - par)
    far = 8 * par
    near_slot, far_slot = 2 * (1 - par), 2 * par

    def parts(start, slot):
        layers = pl.ds(start, 4)
        refs = [fld.at[f, layers, 8:40] for f in range(3)] + [fld.at[f, layers, 4:44] for f in range(3, 4)]
        refs += [msk.at[pl.ds(start, 2), 4:44], msk.at[pl.ds(start + 2, 2), 4:44]]
        refs += [peer.at[slot]]
        return refs

    x_copies = [
        remote(a, b, x_send.at[i], x_recv.at[i], x_peer)
        for i, (a, b) in enumerate(zip(parts(4, 1), parts(far, far_slot)))
    ]
    f_copies = [
        remote(a, b, f_send.at[i], f_recv.at[i], fwd_to)
        for i, (a, b) in enumerate(zip(parts(near, near_slot), parts(far, far_slot)))
    ]
    e_copies = []
    for i, layers in enumerate((pl.ds(near, 4), pl.ds(far, 4))):
        up, down = fld.at[0:3, layers, 36:40], fld.at[0:3, layers, 8:12]
        e_copies += [
            remote(up, fld.at[0:3, layers, 4:8], e_send.at[2 * i], e_recv.at[2 * i], y_up),
            remote(down, fld.at[0:3, layers, 40:44], e_send.at[2 * i + 1], e_recv.at[2 * i + 1], y_down),
        ]
    for c in x_copies[:3]:
        c.start()
    for c in y_copies:
        c.wait_recv()
    for v in range(7):
        acc = None
        for k, m in enumerate(range(3 * v, min(3 * v + 3, 20))):
            part = columns(m // 4, 4 + m % 4)
            part = pltpu.roll(part, 40 * k, 1) if k else part
            acc = part if acc is None else jnp.where(group >= 5 * k, part, acc)
        pack[v] = acc

    def first_four(start):
        def body(i, carry):
            for x in (start + 2 * i, start + 2 * i + 1):
                for r in BLOCKS:
                    rows = slice(r, r + 8)
                    out = first(fld[0, x, rows], fld[1, x, rows], fld[2, x, rows], fld[3, x, rows], msk[x, rows] == 1)
                    for q in range(19):
                        main_a[q, x, rows] = out[q]
            return carry

        lax.fori_loop(0, 2, body, 0)

    def store_side(side, x, out):
        for q, (_, cy, _) in enumerate(VELOCITIES):
            side[q, x, SIDE : SIDE + 8] = out[q]
            if cy == 1:
                side[q, x, SIDE - 1 : SIDE] = pltpu.roll(out[q], 8, 1)[7:8]
            elif cy == -1:
                side[q, x, SIDE + 8 : SIDE + 9] = pltpu.roll(out[q], LANES - 8, 1)[0:1]

    def first_side(start, slot):
        for i in range(4):
            x = start + i
            cells = []
            for f in range(5):
                m = 4 * f + i
                mine = columns(f, x)
                theirs = peer[slot, m // 3]
                theirs = pltpu.roll(theirs, LANES - 40 * (m % 3), 1) if m % 3 else theirs
                above = pltpu.roll(jnp.where(low_half, mine, theirs), 64, 1)
                cells.append(jnp.where(lane < 64, jnp.where(low_half, theirs, mine), above))
            gmsk[x] = cells[4]
            store_side(side_a, x, first(*cells[:4], cells[4] > 0.5))

    def pull_main(main, side, x, b):
        f = []
        r = BLOCKS[b]
        for q, (cx, cy, cz) in enumerate(VELOCITIES):
            value = main[q, x - cx, r - cy : r - cy + 8]
            if cz:
                edge = side[q, x - cx, SIDE - cy : SIDE - cy + 8]
                if cz == 1:
                    edge = pltpu.roll(edge, (125 - 8 * b) % LANES, 1)
                    value = jnp.where(lane == 0, edge, pltpu.roll(value, 1, 1))
                else:
                    edge = pltpu.roll(edge, 59 - 8 * b, 1)
                    value = jnp.where(lane == LANES - 1, edge, pltpu.roll(value, LANES - 1, 1))
            f.append(value)
        return f

    def pull_side(side, x):
        f = []
        for q, (cx, cy, cz) in enumerate(VELOCITIES):
            value = side[q, x - cx, SIDE - cy : SIDE - cy + 8]
            f.append(pltpu.roll(value, cz % LANES, 1) if cz else value)
        return f

    buffers = [(main_a, side_a), (main_b, side_b)]

    def step_layers(step, start, count):
        (main, side), (main_to, side_to) = buffers[step % 2], buffers[(step + 1) % 2]
        unroll = 2

        def body(i, carry):
            x = start + 2 * i + 0
            store_side(side_to, x, collide(pull_side(side, x), gmsk[x] > 0.5))
            x = start + 2 * i + 0
            for b, r in [(b, BLOCKS[b]) for b in [0, 1, 2, 3, 4]]:
                rows = slice(r, r + 8)
                out = collide(pull_main(main, side, x, b), msk[x, rows] == 1)
                for q in range(19):
                    main_to[q, x, rows] = out[q]
            x = start + 2 * i + 1
            for b, r in [(b, BLOCKS[b]) for b in [0, 1, 2, 3, 4]]:
                rows = slice(r, r + 8)
                out = collide(pull_main(main, side, x, b), msk[x, rows] == 1)
                for q in range(19):
                    main_to[q, x, rows] = out[q]
            x = start + 2 * i + 1
            store_side(side_to, x, collide(pull_side(side, x), gmsk[x] > 0.5))
            return carry

        lax.fori_loop(0, count // unroll, body, 0)

    z_copy = remote(pack, peer.at[1], z_send, z_recv, z_peer)
    z_copy.start()
    for c in x_copies[3:6]:
        c.start()
    first_four(4)
    x_copies[0].wait_recv()
    f_copies[0].start()
    x_copies[1].wait_recv()
    f_copies[1].start()
    x_copies[2].wait_recv()
    f_copies[2].start()
    for c in e_copies[:2]:
        c.start()
    z_copy.wait_recv()
    x_copies[6].start()
    x_copies[3].wait_recv()
    f_copies[3].start()
    x_copies[4].wait_recv()
    f_copies[4].start()
    for c in f_copies[:3]:
        c.wait_recv()
    for c in e_copies[2:]:
        c.start()
    x_copies[5].wait_recv()
    f_copies[5].start()
    x_copies[6].wait_recv()
    f_copies[6].start()
    for c in e_copies[:2]:
        c.wait_recv()

    first_side(4, 1)
    first_four(8 - 8 * par)
    first_side(8 - 8 * par, near_slot)
    step_layers(2, 5 - 4 * par, 6)
    step_layers(3, 6 - 4 * par, 4)
    step_layers(4, 7 - 4 * par, 2)

    for c in f_copies[3:6] + e_copies[2:]:
        c.wait_recv()
    first_four(8 * par)
    f_copies[6].wait_recv()
    first_side(8 * par, far_slot)
    step_layers(2, 1 + 6 * par, 4)
    step_layers(3, 2 + 4 * par, 4)
    step_layers(4, 3 + 2 * par, 4)

    def pull(ref, x, row, cz):
        part = {c[:2]: ref[q, x - c[0], row - c[1] : row - c[1] + 8] for q, c in enumerate(VELOCITIES) if c[2] == cz}
        sums = [part[0, 0], part[1, 0] - part[-1, 0], part[0, 1] - part[0, -1]]
        sums[0] += (part[1, 0] + part[-1, 0]) + (part[0, 1] + part[0, -1])
        if not cz:
            diagonal = [part[1, 1], part[-1, -1], part[1, -1], part[-1, 1]]
            sums[0] += (diagonal[0] + diagonal[1]) + (diagonal[2] + diagonal[3])
            sums[1] += (diagonal[0] - diagonal[1]) + (diagonal[2] - diagonal[3])
            sums[2] += (diagonal[0] - diagonal[1]) - (diagonal[2] - diagonal[3])
        return sums

    def moved(x, b, cz):
        row = BLOCKS[b]
        shift, edge_lane = ((125 - 8 * b) % LANES, 0) if cz == 1 else (59 - 8 * b, LANES - 1)
        result = []
        for value, edge in zip(pull(main_b, x, row, cz), pull(side_b, x, SIDE, cz)):
            value = pltpu.roll(value, cz % LANES, 1)
            result.append(jnp.where(lane == edge_lane, pltpu.roll(edge, shift, 1), value))
        return result

    def last(i, carry):
        for x in [4 + 4 * i + k for k in range(4)]:
            for b, r in enumerate(BLOCKS):
                rest, up, down = pull(main_b, x, r, 0), moved(x, b, 1), moved(x, b, -1)
                rho, mx, my = (rest[k] + (up[k] + down[k]) for k in range(3))
                for k, value in enumerate((rho, mx, my, up[0] - down[0])):
                    out[k, x - 4, r : r + 8] = value
        return carry

    lax.fori_loop(0, 4 // 4, last, 0)

    for c in y_copies + [z_copy] + x_copies + f_copies + e_copies:
        c.wait_send()


def split(both, density, momentum, sem):
    copies = [
        pltpu.make_async_copy(both.at[0, :, 8:40], density, sem.at[0]),
        pltpu.make_async_copy(both.at[1:4, :, 8:40], momentum, sem.at[1]),
    ]
    for c in copies:
        c.start()
    for c in copies:
        c.wait()


def local(density, velocity, solid_mask):
    shape = density.shape
    f32 = jnp.float32
    dma = pltpu.SemaphoreType.DMA
    both = pl.pallas_call(
            kernel,
            out_shape=jax.ShapeDtypeStruct((4, shape[0], ROWS, LANES), f32),
            in_specs=[pl.BlockSpec(memory_space=pl.ANY)] * 3,
            out_specs=pl.BlockSpec(memory_space=pltpu.VMEM),
            scratch_shapes=[
                pltpu.VMEM((4, LAYERS, ROWS, LANES), f32),
                pltpu.VMEM((LAYERS, ROWS, LANES), jnp.int32),
                pltpu.VMEM((7, 8, LANES), f32),
                pltpu.VMEM((3, 7, 8, LANES), f32),
                pltpu.VMEM((LAYERS, 8, LANES), f32),
                pltpu.VMEM((19, LAYERS, ROWS, LANES), f32),
                pltpu.VMEM((19, LAYERS, ROWS, LANES), f32),
                pltpu.VMEM((19, LAYERS, 24, LANES), f32),
                pltpu.VMEM((19, LAYERS, 24, LANES), f32),
                dma((3,)),
                dma((4,)),
                dma((4,)),
                dma,
                dma,
                dma((7,)),
                dma((7,)),
                dma((7,)),
                dma((7,)),
                dma((4,)),
                dma((4,)),
            ],
            compiler_params=pltpu.CompilerParams(collective_id=0, has_side_effects=True, vmem_limit_bytes=51043328),
        )(*[pltpu.with_memory_space_constraint(v, pltpu.HBM) for v in (density, velocity, solid_mask)])
    return tuple(
        pl.pallas_call(
            split,
            out_shape=(jax.ShapeDtypeStruct(shape, f32), jax.ShapeDtypeStruct((3,) + shape, f32)),
            in_specs=[pl.BlockSpec(memory_space=pltpu.VMEM)],
            out_specs=(pl.BlockSpec(memory_space=pl.ANY), pl.BlockSpec(memory_space=pl.ANY)),
            scratch_shapes=[dma((2,))],
            compiler_params=pltpu.CompilerParams(vmem_limit_bytes=32 << 20),
        )(both)
    )


def solution(mesh):
    return jax.shard_map(
        local,
        mesh=mesh,
        in_specs=(P("gx", "gy", "gz"), P(None, "gx", "gy", "gz"), P("gx", "gy", "gz")),
        out_specs=(P("gx", "gy", "gz"), P(None, "gx", "gy", "gz")),
        check_vma=False,
    )
```

```python
import jax
import jax.numpy as jnp
from jax import lax
from jax.experimental import pallas as pl
from jax.experimental.pallas import tpu as pltpu
from jax.sharding import PartitionSpec as P

MESH = pl.DeviceIdType.MESH

VELOCITIES = [
    (0, 0, 0),
    (1, 0, 0),
    (-1, 0, 0),
    (0, 1, 0),
    (0, -1, 0),
    (0, 0, 1),
    (0, 0, -1),
    (1, 1, 0),
    (-1, -1, 0),
    (1, -1, 0),
    (-1, 1, 0),
    (1, 0, 1),
    (-1, 0, -1),
    (1, 0, -1),
    (-1, 0, 1),
    (0, 1, 1),
    (0, -1, -1),
    (0, 1, -1),
    (0, -1, 1),
]
RELAX_RATE = 1.25
W0, W1, W2 = 1.0 / 3.0, 1.0 / 18.0, 1.0 / 36.0

LAYERS, ROWS, LANES = 12, 48, 128
BLOCKS = [4 + 8 * j for j in range(5)]
SIDE = 8


def moments(f):
    s = [f[2 * k + 1] + f[2 * k + 2] for k in range(9)]
    d = [f[2 * k + 1] - f[2 * k + 2] for k in range(9)]
    rho = f[0] + (((s[0] + s[1]) + (s[2] + s[3])) + ((s[4] + s[5]) + (s[6] + s[7]))) + s[8]
    mx = d[0] + (d[3] + d[4]) + (d[5] + d[6])
    my = d[1] + (d[3] - d[4]) + (d[7] + d[8])
    mz = d[2] + (d[5] - d[6]) + (d[7] - d[8])
    return rho, (mx, my, mz), s, d


def balance(rho, m, u, scale):
    mx, my, mz = m
    ux, uy, uz = u
    xx, yy, zz = mx * ux, my * uy, mz * uz
    base = (scale * W2) * rho - (1.0 / 3.0) * (xx + yy + zz)
    px, py, pz = (scale * W2 * 3.0) * mx, (scale * W2 * 3.0) * my, (scale * W2 * 3.0) * mz
    ax, ay, az = base + xx, base + yy, base + zz
    pairs = [(ax + ax, px + px), (ay + ay, py + py), (az + az, pz + pz)]
    mx2, my2 = mx + mx, my + my
    for even, cross, pa, pb in (
        (ax + yy, mx2 * uy, px, py),
        (ax + zz, mx2 * uz, px, pz),
        (ay + zz, my2 * uz, py, pz),
    ):
        pairs.append((even + cross, pa + pb))
        pairs.append((even - cross, pa - pb))
    return (W0 / W2) * base, pairs


def first(rho, vx, vy, vz, solid):
    sign = jnp.where(solid, -1.0, 1.0)
    m = tuple((rho * sign) * v for v in (vx, vy, vz))
    half = jnp.where(solid, -W2 * 4.5, W2 * 4.5)
    rest, pairs = balance(rho, m, tuple(half * v for v in (vx, vy, vz)), 1.0)
    out = [rest]
    for even, odd in pairs:
        out += [even + odd, even - odd]
    return out


def collide(f, solid):
    rho, m, s, d = moments(f)
    inv = (RELAX_RATE * W2 * 4.5) / rho
    u = tuple(v * inv for v in m)
    rho, *m = (jnp.where(solid, 0.0, v) for v in (rho, *m))
    rest, pairs = balance(rho, m, u, RELAX_RATE)
    keep = 1.0 - RELAX_RATE
    keep_rest = jnp.where(solid, 1.0, keep)
    keep_sum = jnp.where(solid, 0.5, 0.5 * keep)
    keep_diff = jnp.where(solid, -0.5, 0.5 * keep)
    out = [keep_rest * f[0] + rest]
    for k, (even, odd) in enumerate(pairs):
        even = even + keep_sum * s[k]
        odd = odd + keep_diff * d[k]
        out += [even + odd, even - odd]
    return out


def kernel(
    density,
    velocity,
    mask,
    out,
    fld,
    msk,
    pack,
    peer,
    gmsk,
    main_a,
    main_b,
    side_a,
    side_b,
    load_sem,
    y_send,
    y_recv,
    z_send,
    z_recv,
    x_send,
    x_recv,
    f_send,
    f_recv,
    e_send,
    e_recv,
):
    gx, gy, gz = lax.axis_index("gx"), lax.axis_index("gy"), lax.axis_index("gz")
    par = lax.rem(gx, 2)
    y_up = (gx, lax.rem(gy + 1, 8), gz)
    y_down = (gx, lax.rem(gy + 7, 8), gz)
    z_peer = (gx, gy, 1 - gz)
    x_peer = (gx + 1 - 2 * par, gy, gz)
    fwd_to = (lax.rem(gx + 2 + 4 * par, 8), gy, gz)
    fwd_from = (lax.rem(gx + 6 - 4 * par, 8), gy, gz)

    loads = [
        pltpu.make_async_copy(density, fld.at[0, 4:8, 8:40], load_sem.at[0]),
        pltpu.make_async_copy(velocity, fld.at[1:4, 4:8, 8:40], load_sem.at[1]),
        pltpu.make_async_copy(mask, msk.at[4:8, 8:40], load_sem.at[2]),
    ]
    for c in loads:
        c.start()

    barrier = pltpu.get_barrier_semaphore()
    for dev in (y_up, y_down, z_peer, x_peer, fwd_to, fwd_from):
        pl.semaphore_signal(barrier, inc=1, device_id=dev, device_id_type=MESH)

    lane = lax.broadcasted_iota(jnp.int32, (8, LANES), 1)
    group = lane // 8
    low_half = lax.rem(lane, 8) < 4

    def field_rows(f, x, r):
        return fld[f, x, r : r + 8] if f < 4 else msk[x, r : r + 8].astype(jnp.float32)

    def columns(f, x):
        acc = None
        for b, r in enumerate(BLOCKS):
            part = pltpu.roll(field_rows(f, x, r), 8 * b + 4, 1)
            acc = part if acc is None else jnp.where(group == b, part, acc)
        return acc

    for c in loads:
        c.wait()
    pl.semaphore_wait(barrier, 6)

    def remote(src, dst, send, recv, dev):
        return pltpu.make_async_remote_copy(
            src_ref=src, dst_ref=dst, send_sem=send, recv_sem=recv, device_id=dev, device_id_type=MESH
        )

    y_copies = [
        remote(fld.at[:, 4:8, 36:40], fld.at[:, 4:8, 4:8], y_send.at[0], y_recv.at[0], y_up),
        remote(fld.at[:, 4:8, 8:12], fld.at[:, 4:8, 40:44], y_send.at[1], y_recv.at[1], y_down),
        remote(msk.at[4:8, 36:40], msk.at[4:8, 4:8], y_send.at[2], y_recv.at[2], y_up),
        remote(msk.at[4:8, 8:12], msk.at[4:8, 40:44], y_send.at[3], y_recv.at[3], y_down),
    ]
    for c in y_copies:
        c.start()

    near = 8 * (1 - par)
    far = 8 * par
    near_slot, far_slot = 2 * (1 - par), 2 * par

    def parts(start, slot):
        layers = pl.ds(start, 4)
        refs = [fld.at[f, layers, 8:40] for f in range(3)] + [fld.at[f, layers, 4:44] for f in range(3, 4)]
        refs += [msk.at[pl.ds(start, 2), 4:44], msk.at[pl.ds(start + 2, 2), 4:44]]
        refs += [peer.at[slot]]
        return refs

    x_copies = [
        remote(a, b, x_send.at[i], x_recv.at[i], x_peer)
        for i, (a, b) in enumerate(zip(parts(4, 1), parts(far, far_slot)))
    ]
    f_copies = [
        remote(a, b, f_send.at[i], f_recv.at[i], fwd_to)
        for i, (a, b) in enumerate(zip(parts(near, near_slot), parts(far, far_slot)))
    ]
    e_copies = []
    for i, layers in enumerate((pl.ds(near, 4), pl.ds(far, 4))):
        up, down = fld.at[0:3, layers, 36:40], fld.at[0:3, layers, 8:12]
        e_copies += [
            remote(up, fld.at[0:3, layers, 4:8], e_send.at[2 * i], e_recv.at[2 * i], y_up),
            remote(down, fld.at[0:3, layers, 40:44], e_send.at[2 * i + 1], e_recv.at[2 * i + 1], y_down),
        ]
    for c in x_copies[:3]:
        c.start()
    for c in y_copies:
        c.wait_recv()
    for v in range(7):
        acc = None
        for k, m in enumerate(range(3 * v, min(3 * v + 3, 20))):
            part = columns(m // 4, 4 + m % 4)
            part = pltpu.roll(part, 40 * k, 1) if k else part
            acc = part if acc is None else jnp.where(group >= 5 * k, part, acc)
        pack[v] = acc

    def first_four(start):
        def body(i, carry):
            for x in (start + 2 * i, start + 2 * i + 1):
                for r in BLOCKS:
                    rows = slice(r, r + 8)
                    out = first(fld[0, x, rows], fld[1, x, rows], fld[2, x, rows], fld[3, x, rows], msk[x, rows] == 1)
                    for q in range(19):
                        main_a[q, x, rows] = out[q]
            return carry

        lax.fori_loop(0, 2, body, 0)

    def store_side(side, x, out):
        for q, (_, cy, _) in enumerate(VELOCITIES):
            side[q, x, SIDE : SIDE + 8] = out[q]
            if cy == 1:
                side[q, x, SIDE - 1 : SIDE] = pltpu.roll(out[q], 8, 1)[7:8]
            elif cy == -1:
                side[q, x, SIDE + 8 : SIDE + 9] = pltpu.roll(out[q], LANES - 8, 1)[0:1]

    def first_side(start, slot):
        for i in range(4):
            x = start + i
            cells = []
            for f in range(5):
                m = 4 * f + i
                mine = columns(f, x)
                theirs = peer[slot, m // 3]
                theirs = pltpu.roll(theirs, LANES - 40 * (m % 3), 1) if m % 3 else theirs
                above = pltpu.roll(jnp.where(low_half, mine, theirs), 64, 1)
                cells.append(jnp.where(lane < 64, jnp.where(low_half, theirs, mine), above))
            gmsk[x] = cells[4]
            store_side(side_a, x, first(*cells[:4], cells[4] > 0.5))

    def pull_main(main, side, x, b):
        f = []
        r = BLOCKS[b]
        for q, (cx, cy, cz) in enumerate(VELOCITIES):
            value = main[q, x - cx, r - cy : r - cy + 8]
            if cz:
                edge = side[q, x - cx, SIDE - cy : SIDE - cy + 8]
                if cz == 1:
                    edge = pltpu.roll(edge, (125 - 8 * b) % LANES, 1)
                    value = jnp.where(lane == 0, edge, pltpu.roll(value, 1, 1))
                else:
                    edge = pltpu.roll(edge, 59 - 8 * b, 1)
                    value = jnp.where(lane == LANES - 1, edge, pltpu.roll(value, LANES - 1, 1))
            f.append(value)
        return f

    def pull_side(side, x):
        f = []
        for q, (cx, cy, cz) in enumerate(VELOCITIES):
            value = side[q, x - cx, SIDE - cy : SIDE - cy + 8]
            f.append(pltpu.roll(value, cz % LANES, 1) if cz else value)
        return f

    buffers = [(main_a, side_a), (main_b, side_b)]

    def step_layers(step, start, count):
        (main, side), (main_to, side_to) = buffers[step % 2], buffers[(step + 1) % 2]
        unroll = 2

        def body(i, carry):
            x = start + 2 * i + 0
            store_side(side_to, x, collide(pull_side(side, x), gmsk[x] > 0.5))
            x = start + 2 * i + 0
            for b, r in [(b, BLOCKS[b]) for b in [0, 1, 2, 3, 4]]:
                rows = slice(r, r + 8)
                out = collide(pull_main(main, side, x, b), msk[x, rows] == 1)
                for q in range(19):
                    main_to[q, x, rows] = out[q]
            x = start + 2 * i + 1
            for b, r in [(b, BLOCKS[b]) for b in [0, 1, 2, 3, 4]]:
                rows = slice(r, r + 8)
                out = collide(pull_main(main, side, x, b), msk[x, rows] == 1)
                for q in range(19):
                    main_to[q, x, rows] = out[q]
            x = start + 2 * i + 1
            store_side(side_to, x, collide(pull_side(side, x), gmsk[x] > 0.5))
            return carry

        lax.fori_loop(0, count // unroll, body, 0)

    z_copy = remote(pack, peer.at[1], z_send, z_recv, z_peer)
    z_copy.start()
    for c in x_copies[3:6]:
        c.start()
    first_four(4)
    x_copies[0].wait_recv()
    f_copies[0].start()
    x_copies[1].wait_recv()
    f_copies[1].start()
    x_copies[2].wait_recv()
    f_copies[2].start()
    for c in e_copies[:2]:
        c.start()
    z_copy.wait_recv()
    x_copies[6].start()
    first_side(4, 1)
    x_copies[3].wait_recv()
    f_copies[3].start()
    x_copies[4].wait_recv()
    f_copies[4].start()
    for c in f_copies[:3]:
        c.wait_recv()
    for c in e_copies[2:]:
        c.start()
    x_copies[5].wait_recv()
    f_copies[5].start()
    x_copies[6].wait_recv()
    f_copies[6].start()
    for c in e_copies[:2]:
        c.wait_recv()

    first_four(8 - 8 * par)
    first_side(8 - 8 * par, near_slot)
    step_layers(2, 5 - 4 * par, 6)
    step_layers(3, 6 - 4 * par, 4)
    step_layers(4, 7 - 4 * par, 2)

    for c in f_copies[3:6] + e_copies[2:]:
        c.wait_recv()
    first_four(8 * par)
    f_copies[6].wait_recv()
    first_side(8 * par, far_slot)
    step_layers(2, 1 + 6 * par, 4)
    step_layers(3, 2 + 4 * par, 4)
    step_layers(4, 3 + 2 * par, 4)

    def pull(ref, x, row, cz):
        part = {c[:2]: ref[q, x - c[0], row - c[1] : row - c[1] + 8] for q, c in enumerate(VELOCITIES) if c[2] == cz}
        sums = [part[0, 0], part[1, 0] - part[-1, 0], part[0, 1] - part[0, -1]]
        sums[0] += (part[1, 0] + part[-1, 0]) + (part[0, 1] + part[0, -1])
        if not cz:
            diagonal = [part[1, 1], part[-1, -1], part[1, -1], part[-1, 1]]
            sums[0] += (diagonal[0] + diagonal[1]) + (diagonal[2] + diagonal[3])
            sums[1] += (diagonal[0] - diagonal[1]) + (diagonal[2] - diagonal[3])
            sums[2] += (diagonal[0] - diagonal[1]) - (diagonal[2] - diagonal[3])
        return sums

    def moved(x, b, cz):
        row = BLOCKS[b]
        shift, edge_lane = ((125 - 8 * b) % LANES, 0) if cz == 1 else (59 - 8 * b, LANES - 1)
        result = []
        for value, edge in zip(pull(main_b, x, row, cz), pull(side_b, x, SIDE, cz)):
            value = pltpu.roll(value, cz % LANES, 1)
            result.append(jnp.where(lane == edge_lane, pltpu.roll(edge, shift, 1), value))
        return result

    def last(i, carry):
        for x in [4 + 4 * i + k for k in range(4)]:
            for b, r in enumerate(BLOCKS):
                rest, up, down = pull(main_b, x, r, 0), moved(x, b, 1), moved(x, b, -1)
                rho, mx, my = (rest[k] + (up[k] + down[k]) for k in range(3))
                for k, value in enumerate((rho, mx, my, up[0] - down[0])):
                    out[k, x - 4, r : r + 8] = value
        return carry

    lax.fori_loop(0, 4 // 4, last, 0)

    for c in y_copies + [z_copy] + x_copies + f_copies + e_copies:
        c.wait_send()


def split(both, density, momentum, sem):
    copies = [
        pltpu.make_async_copy(both.at[0, :, 8:40], density, sem.at[0]),
        pltpu.make_async_copy(both.at[1:4, :, 8:40], momentum, sem.at[1]),
    ]
    for c in copies:
        c.start()
    for c in copies:
        c.wait()


def local(density, velocity, solid_mask):
    shape = density.shape
    f32 = jnp.float32
    dma = pltpu.SemaphoreType.DMA
    both = pl.pallas_call(
            kernel,
            out_shape=jax.ShapeDtypeStruct((4, shape[0], ROWS, LANES), f32),
            in_specs=[pl.BlockSpec(memory_space=pl.ANY)] * 3,
            out_specs=pl.BlockSpec(memory_space=pltpu.VMEM),
            scratch_shapes=[
                pltpu.VMEM((4, LAYERS, ROWS, LANES), f32),
                pltpu.VMEM((LAYERS, ROWS, LANES), jnp.int32),
                pltpu.VMEM((7, 8, LANES), f32),
                pltpu.VMEM((3, 7, 8, LANES), f32),
                pltpu.VMEM((LAYERS, 8, LANES), f32),
                pltpu.VMEM((19, LAYERS, ROWS, LANES), f32),
                pltpu.VMEM((19, LAYERS, ROWS, LANES), f32),
                pltpu.VMEM((19, LAYERS, 24, LANES), f32),
                pltpu.VMEM((19, LAYERS, 24, LANES), f32),
                dma((3,)),
                dma((4,)),
                dma((4,)),
                dma,
                dma,
                dma((7,)),
                dma((7,)),
                dma((7,)),
                dma((7,)),
                dma((4,)),
                dma((4,)),
            ],
            compiler_params=pltpu.CompilerParams(collective_id=0, has_side_effects=True, vmem_limit_bytes=51043328),
        )(*[pltpu.with_memory_space_constraint(v, pltpu.HBM) for v in (density, velocity, solid_mask)])
    return tuple(
        pl.pallas_call(
            split,
            out_shape=(jax.ShapeDtypeStruct(shape, f32), jax.ShapeDtypeStruct((3,) + shape, f32)),
            in_specs=[pl.BlockSpec(memory_space=pltpu.VMEM)],
            out_specs=(pl.BlockSpec(memory_space=pl.ANY), pl.BlockSpec(memory_space=pl.ANY)),
            scratch_shapes=[dma((2,))],
            compiler_params=pltpu.CompilerParams(vmem_limit_bytes=32 << 20),
        )(both)
    )


def solution(mesh):
    return jax.shard_map(
        local,
        mesh=mesh,
        in_specs=(P("gx", "gy", "gz"), P(None, "gx", "gy", "gz"), P("gx", "gy", "gz")),
        out_specs=(P("gx", "gy", "gz"), P(None, "gx", "gy", "gz")),
        check_vma=False,
    )
```

```python
import jax
import jax.numpy as jnp
from jax import lax
from jax.experimental import pallas as pl
from jax.experimental.pallas import tpu as pltpu
from jax.sharding import PartitionSpec as P

MESH = pl.DeviceIdType.MESH

VELOCITIES = [
    (0, 0, 0),
    (1, 0, 0),
    (-1, 0, 0),
    (0, 1, 0),
    (0, -1, 0),
    (0, 0, 1),
    (0, 0, -1),
    (1, 1, 0),
    (-1, -1, 0),
    (1, -1, 0),
    (-1, 1, 0),
    (1, 0, 1),
    (-1, 0, -1),
    (1, 0, -1),
    (-1, 0, 1),
    (0, 1, 1),
    (0, -1, -1),
    (0, 1, -1),
    (0, -1, 1),
]
RELAX_RATE = 1.25
W0, W1, W2 = 1.0 / 3.0, 1.0 / 18.0, 1.0 / 36.0

LAYERS, ROWS, LANES = 12, 48, 128
BLOCKS = [4 + 8 * j for j in range(5)]
SIDE = 8


def moments(f):
    s = [f[2 * k + 1] + f[2 * k + 2] for k in range(9)]
    d = [f[2 * k + 1] - f[2 * k + 2] for k in range(9)]
    rho = f[0] + (((s[0] + s[1]) + (s[2] + s[3])) + ((s[4] + s[5]) + (s[6] + s[7]))) + s[8]
    mx = d[0] + (d[3] + d[4]) + (d[5] + d[6])
    my = d[1] + (d[3] - d[4]) + (d[7] + d[8])
    mz = d[2] + (d[5] - d[6]) + (d[7] - d[8])
    return rho, (mx, my, mz), s, d


def balance(rho, m, u, scale):
    mx, my, mz = m
    ux, uy, uz = u
    xx, yy, zz = mx * ux, my * uy, mz * uz
    base = (scale * W2) * rho - (1.0 / 3.0) * (xx + yy + zz)
    px, py, pz = (scale * W2 * 3.0) * mx, (scale * W2 * 3.0) * my, (scale * W2 * 3.0) * mz
    ax, ay, az = base + xx, base + yy, base + zz
    pairs = [(ax + ax, px + px), (ay + ay, py + py), (az + az, pz + pz)]
    mx2, my2 = mx + mx, my + my
    for even, cross, pa, pb in (
        (ax + yy, mx2 * uy, px, py),
        (ax + zz, mx2 * uz, px, pz),
        (ay + zz, my2 * uz, py, pz),
    ):
        pairs.append((even + cross, pa + pb))
        pairs.append((even - cross, pa - pb))
    return (W0 / W2) * base, pairs


def first(rho, vx, vy, vz, solid):
    sign = jnp.where(solid, -1.0, 1.0)
    m = tuple((rho * sign) * v for v in (vx, vy, vz))
    half = jnp.where(solid, -W2 * 4.5, W2 * 4.5)
    rest, pairs = balance(rho, m, tuple(half * v for v in (vx, vy, vz)), 1.0)
    out = [rest]
    for even, odd in pairs:
        out += [even + odd, even - odd]
    return out


def collide(f, solid):
    rho, m, s, d = moments(f)
    inv = (RELAX_RATE * W2 * 4.5) / rho
    u = tuple(v * inv for v in m)
    rho, *m = (jnp.where(solid, 0.0, v) for v in (rho, *m))
    rest, pairs = balance(rho, m, u, RELAX_RATE)
    keep = 1.0 - RELAX_RATE
    keep_rest = jnp.where(solid, 1.0, keep)
    keep_sum = jnp.where(solid, 0.5, 0.5 * keep)
    keep_diff = jnp.where(solid, -0.5, 0.5 * keep)
    out = [keep_rest * f[0] + rest]
    for k, (even, odd) in enumerate(pairs):
        even = even + keep_sum * s[k]
        odd = odd + keep_diff * d[k]
        out += [even + odd, even - odd]
    return out


def kernel(
    density,
    velocity,
    mask,
    out,
    fld,
    msk,
    pack,
    peer,
    cols,
    gmsk,
    main_a,
    main_b,
    side_a,
    side_b,
    load_sem,
    y_send,
    y_recv,
    z_send,
    z_recv,
    x_send,
    x_recv,
    f_send,
    f_recv,
    e_send,
    e_recv,
):
    gx, gy, gz = lax.axis_index("gx"), lax.axis_index("gy"), lax.axis_index("gz")
    par = lax.rem(gx, 2)
    y_up = (gx, lax.rem(gy + 1, 8), gz)
    y_down = (gx, lax.rem(gy + 7, 8), gz)
    z_peer = (gx, gy, 1 - gz)
    x_peer = (gx + 1 - 2 * par, gy, gz)
    fwd_to = (lax.rem(gx + 2 + 4 * par, 8), gy, gz)
    fwd_from = (lax.rem(gx + 6 - 4 * par, 8), gy, gz)

    loads = [
        pltpu.make_async_copy(density, fld.at[0, 4:8, 8:40], load_sem.at[0]),
        pltpu.make_async_copy(velocity, fld.at[1:4, 4:8, 8:40], load_sem.at[1]),
        pltpu.make_async_copy(mask, msk.at[4:8, 8:40], load_sem.at[2]),
    ]
    for c in loads:
        c.start()

    barrier = pltpu.get_barrier_semaphore()
    for dev in (y_up, y_down, z_peer, x_peer, fwd_to, fwd_from):
        pl.semaphore_signal(barrier, inc=1, device_id=dev, device_id_type=MESH)

    lane = lax.broadcasted_iota(jnp.int32, (8, LANES), 1)
    group = lane // 8
    low_half = lax.rem(lane, 8) < 4

    def field_rows(f, x, r):
        return fld[f, x, r : r + 8] if f < 4 else msk[x, r : r + 8].astype(jnp.float32)

    def columns(f, x):
        acc = None
        for b, r in enumerate(BLOCKS):
            part = pltpu.roll(field_rows(f, x, r), 8 * b + 4, 1)
            acc = part if acc is None else jnp.where(group == b, part, acc)
        return acc

    for c in loads:
        c.wait()
    pl.semaphore_wait(barrier, 6)

    def remote(src, dst, send, recv, dev):
        return pltpu.make_async_remote_copy(
            src_ref=src, dst_ref=dst, send_sem=send, recv_sem=recv, device_id=dev, device_id_type=MESH
        )

    y_copies = [
        remote(fld.at[:, 4:8, 36:40], fld.at[:, 4:8, 4:8], y_send.at[0], y_recv.at[0], y_up),
        remote(fld.at[:, 4:8, 8:12], fld.at[:, 4:8, 40:44], y_send.at[1], y_recv.at[1], y_down),
        remote(msk.at[4:8, 36:40], msk.at[4:8, 4:8], y_send.at[2], y_recv.at[2], y_up),
        remote(msk.at[4:8, 8:12], msk.at[4:8, 40:44], y_send.at[3], y_recv.at[3], y_down),
    ]
    for c in y_copies:
        c.start()

    near = 8 * (1 - par)
    far = 8 * par
    near_slot, far_slot = 2 * (1 - par), 2 * par

    def parts(start, slot):
        layers = pl.ds(start, 4)
        refs = [fld.at[f, layers, 8:40] for f in range(3)] + [fld.at[f, layers, 4:44] for f in range(3, 4)]
        refs += [msk.at[pl.ds(start, 2), 4:44], msk.at[pl.ds(start + 2, 2), 4:44]]
        refs += [peer.at[slot]]
        return refs

    x_copies = [
        remote(a, b, x_send.at[i], x_recv.at[i], x_peer)
        for i, (a, b) in enumerate(zip(parts(4, 1), parts(far, far_slot)))
    ]
    f_copies = [
        remote(a, b, f_send.at[i], f_recv.at[i], fwd_to)
        for i, (a, b) in enumerate(zip(parts(near, near_slot), parts(far, far_slot)))
    ]
    e_copies = []
    for i, layers in enumerate((pl.ds(near, 4), pl.ds(far, 4))):
        up, down = fld.at[0:3, layers, 36:40], fld.at[0:3, layers, 8:12]
        e_copies += [
            remote(up, fld.at[0:3, layers, 4:8], e_send.at[2 * i], e_recv.at[2 * i], y_up),
            remote(down, fld.at[0:3, layers, 40:44], e_send.at[2 * i + 1], e_recv.at[2 * i + 1], y_down),
        ]
    for c in x_copies[:3]:
        c.start()
    for c in y_copies:
        c.wait_recv()
    for v in range(7):
        acc = None
        for k, m in enumerate(range(3 * v, min(3 * v + 3, 20))):
            part = columns(m // 4, 4 + m % 4)
            cols[1, m] = part
            part = pltpu.roll(part, 40 * k, 1) if k else part
            acc = part if acc is None else jnp.where(group >= 5 * k, part, acc)
        pack[v] = acc

    def first_four(start):
        def body(i, carry):
            for x in (start + 2 * i, start + 2 * i + 1):
                for r in BLOCKS:
                    rows = slice(r, r + 8)
                    out = first(fld[0, x, rows], fld[1, x, rows], fld[2, x, rows], fld[3, x, rows], msk[x, rows] == 1)
                    for q in range(19):
                        main_a[q, x, rows] = out[q]
            return carry

        lax.fori_loop(0, 2, body, 0)

    def store_side(side, x, out):
        for q, (_, cy, _) in enumerate(VELOCITIES):
            side[q, x, SIDE : SIDE + 8] = out[q]
            if cy == 1:
                side[q, x, SIDE - 1 : SIDE] = pltpu.roll(out[q], 8, 1)[7:8]
            elif cy == -1:
                side[q, x, SIDE + 8 : SIDE + 9] = pltpu.roll(out[q], LANES - 8, 1)[0:1]

    def side_columns(start, slot):
        for m in range(20):
            cols[slot, m] = columns(m // 4, start + m % 4)

    def first_side(start, slot):
        for i in range(4):
            x = start + i
            cells = []
            for f in range(5):
                m = 4 * f + i
                mine = cols[slot, m]
                theirs = peer[slot, m // 3]
                theirs = pltpu.roll(theirs, LANES - 40 * (m % 3), 1) if m % 3 else theirs
                above = pltpu.roll(jnp.where(low_half, mine, theirs), 64, 1)
                cells.append(jnp.where(lane < 64, jnp.where(low_half, theirs, mine), above))
            gmsk[x] = cells[4]
            store_side(side_a, x, first(*cells[:4], cells[4] > 0.5))

    def pull_main(main, side, x, b):
        f = []
        r = BLOCKS[b]
        for q, (cx, cy, cz) in enumerate(VELOCITIES):
            value = main[q, x - cx, r - cy : r - cy + 8]
            if cz:
                edge = side[q, x - cx, SIDE - cy : SIDE - cy + 8]
                if cz == 1:
                    edge = pltpu.roll(edge, (125 - 8 * b) % LANES, 1)
                    value = jnp.where(lane == 0, edge, pltpu.roll(value, 1, 1))
                else:
                    edge = pltpu.roll(edge, 59 - 8 * b, 1)
                    value = jnp.where(lane == LANES - 1, edge, pltpu.roll(value, LANES - 1, 1))
            f.append(value)
        return f

    def pull_side(side, x):
        f = []
        for q, (cx, cy, cz) in enumerate(VELOCITIES):
            value = side[q, x - cx, SIDE - cy : SIDE - cy + 8]
            f.append(pltpu.roll(value, cz % LANES, 1) if cz else value)
        return f

    buffers = [(main_a, side_a), (main_b, side_b)]

    def step_layers(step, start, count):
        (main, side), (main_to, side_to) = buffers[step % 2], buffers[(step + 1) % 2]
        unroll = 2

        def body(i, carry):
            x = start + 2 * i + 0
            store_side(side_to, x, collide(pull_side(side, x), gmsk[x] > 0.5))
            x = start + 2 * i + 0
            for b, r in [(b, BLOCKS[b]) for b in [0, 1, 2, 3, 4]]:
                rows = slice(r, r + 8)
                out = collide(pull_main(main, side, x, b), msk[x, rows] == 1)
                for q in range(19):
                    main_to[q, x, rows] = out[q]
            x = start + 2 * i + 1
            for b, r in [(b, BLOCKS[b]) for b in [0, 1, 2, 3, 4]]:
                rows = slice(r, r + 8)
                out = collide(pull_main(main, side, x, b), msk[x, rows] == 1)
                for q in range(19):
                    main_to[q, x, rows] = out[q]
            x = start + 2 * i + 1
            store_side(side_to, x, collide(pull_side(side, x), gmsk[x] > 0.5))
            return carry

        lax.fori_loop(0, count // unroll, body, 0)

    z_copy = remote(pack, peer.at[1], z_send, z_recv, z_peer)
    z_copy.start()
    for c in x_copies[3:6]:
        c.start()
    first_four(4)
    x_copies[0].wait_recv()
    f_copies[0].start()
    x_copies[1].wait_recv()
    f_copies[1].start()
    x_copies[2].wait_recv()
    f_copies[2].start()
    for c in e_copies[:2]:
        c.start()
    z_copy.wait_recv()
    x_copies[6].start()
    x_copies[3].wait_recv()
    f_copies[3].start()
    x_copies[4].wait_recv()
    f_copies[4].start()
    for c in f_copies[:3]:
        c.wait_recv()
    for c in e_copies[2:]:
        c.start()
    x_copies[5].wait_recv()
    f_copies[5].start()
    x_copies[6].wait_recv()
    f_copies[6].start()
    for c in e_copies[:2]:
        c.wait_recv()

    first_side(4, 1)
    first_four(8 - 8 * par)
    side_columns(8 - 8 * par, near_slot)
    first_side(8 - 8 * par, near_slot)
    step_layers(2, 5 - 4 * par, 6)
    step_layers(3, 6 - 4 * par, 4)
    step_layers(4, 7 - 4 * par, 2)

    for c in f_copies[3:6] + e_copies[2:]:
        c.wait_recv()
    first_four(8 * par)
    side_columns(8 * par, far_slot)
    f_copies[6].wait_recv()
    first_side(8 * par, far_slot)
    step_layers(2, 1 + 6 * par, 4)
    step_layers(3, 2 + 4 * par, 4)
    step_layers(4, 3 + 2 * par, 4)

    def pull(ref, x, row, cz):
        part = {c[:2]: ref[q, x - c[0], row - c[1] : row - c[1] + 8] for q, c in enumerate(VELOCITIES) if c[2] == cz}
        sums = [part[0, 0], part[1, 0] - part[-1, 0], part[0, 1] - part[0, -1]]
        sums[0] += (part[1, 0] + part[-1, 0]) + (part[0, 1] + part[0, -1])
        if not cz:
            diagonal = [part[1, 1], part[-1, -1], part[1, -1], part[-1, 1]]
            sums[0] += (diagonal[0] + diagonal[1]) + (diagonal[2] + diagonal[3])
            sums[1] += (diagonal[0] - diagonal[1]) + (diagonal[2] - diagonal[3])
            sums[2] += (diagonal[0] - diagonal[1]) - (diagonal[2] - diagonal[3])
        return sums

    def moved(x, b, cz):
        row = BLOCKS[b]
        shift, edge_lane = ((125 - 8 * b) % LANES, 0) if cz == 1 else (59 - 8 * b, LANES - 1)
        result = []
        for value, edge in zip(pull(main_b, x, row, cz), pull(side_b, x, SIDE, cz)):
            value = pltpu.roll(value, cz % LANES, 1)
            result.append(jnp.where(lane == edge_lane, pltpu.roll(edge, shift, 1), value))
        return result

    def last(i, carry):
        for x in [4 + 4 * i + k for k in range(4)]:
            for b, r in enumerate(BLOCKS):
                rest, up, down = pull(main_b, x, r, 0), moved(x, b, 1), moved(x, b, -1)
                rho, mx, my = (rest[k] + (up[k] + down[k]) for k in range(3))
                for k, value in enumerate((rho, mx, my, up[0] - down[0])):
                    out[k, x - 4, r : r + 8] = value
        return carry

    lax.fori_loop(0, 4 // 4, last, 0)

    for c in y_copies + [z_copy] + x_copies + f_copies + e_copies:
        c.wait_send()


def split(both, density, momentum, sem):
    copies = [
        pltpu.make_async_copy(both.at[0, :, 8:40], density, sem.at[0]),
        pltpu.make_async_copy(both.at[1:4, :, 8:40], momentum, sem.at[1]),
    ]
    for c in copies:
        c.start()
    for c in copies:
        c.wait()


def local(density, velocity, solid_mask):
    shape = density.shape
    f32 = jnp.float32
    dma = pltpu.SemaphoreType.DMA
    both = pl.pallas_call(
            kernel,
            out_shape=jax.ShapeDtypeStruct((4, shape[0], ROWS, LANES), f32),
            in_specs=[pl.BlockSpec(memory_space=pl.ANY)] * 3,
            out_specs=pl.BlockSpec(memory_space=pltpu.VMEM),
            scratch_shapes=[
                pltpu.VMEM((4, LAYERS, ROWS, LANES), f32),
                pltpu.VMEM((LAYERS, ROWS, LANES), jnp.int32),
                pltpu.VMEM((7, 8, LANES), f32),
                pltpu.VMEM((3, 7, 8, LANES), f32),
                pltpu.VMEM((3, 20, 8, LANES), f32),
                pltpu.VMEM((LAYERS, 8, LANES), f32),
                pltpu.VMEM((19, LAYERS, ROWS, LANES), f32),
                pltpu.VMEM((19, LAYERS, ROWS, LANES), f32),
                pltpu.VMEM((19, LAYERS, 24, LANES), f32),
                pltpu.VMEM((19, LAYERS, 24, LANES), f32),
                dma((3,)),
                dma((4,)),
                dma((4,)),
                dma,
                dma,
                dma((7,)),
                dma((7,)),
                dma((7,)),
                dma((7,)),
                dma((4,)),
                dma((4,)),
            ],
            compiler_params=pltpu.CompilerParams(collective_id=0, has_side_effects=True, vmem_limit_bytes=51043328),
        )(*[pltpu.with_memory_space_constraint(v, pltpu.HBM) for v in (density, velocity, solid_mask)])
    return tuple(
        pl.pallas_call(
            split,
            out_shape=(jax.ShapeDtypeStruct(shape, f32), jax.ShapeDtypeStruct((3,) + shape, f32)),
            in_specs=[pl.BlockSpec(memory_space=pltpu.VMEM)],
            out_specs=(pl.BlockSpec(memory_space=pl.ANY), pl.BlockSpec(memory_space=pl.ANY)),
            scratch_shapes=[dma((2,))],
            compiler_params=pltpu.CompilerParams(vmem_limit_bytes=32 << 20),
        )(both)
    )


def solution(mesh):
    return jax.shard_map(
        local,
        mesh=mesh,
        in_specs=(P("gx", "gy", "gz"), P(None, "gx", "gy", "gz"), P("gx", "gy", "gz")),
        out_specs=(P("gx", "gy", "gz"), P(None, "gx", "gy", "gz")),
        check_vma=False,
    )
```
